32 devices in a mesh: dp: 4 (over x, core), hist: 8 (over z, y).
Axes of the slice: x: 2, y: 2, z: 4, core: 2. Of those that a mesh axis runs over, the one named last changes fastest.
Arguments:
- candidates: bfloat16 [16, 512, 128], P('dp', 'hist'), may hold values from -150 to 150
- history: bfloat16 [16, 16384, 128], P('dp', 'hist'), may hold values from -6 to 6
- projections: bfloat16 [4, 128, 128], P(None, 'dp'), may hold values from -0.5 to 0.5
- lengths: int32 [16], P('dp'), may hold values from 8193 to 16384
- selected: int32 [16, 64], P('dp'), may hold values from 0 to 127, as said below
Outputs:
- interest: bfloat16 [16, 512, 128], P('dp', 'hist')
The draws below stay inside these ranges and needn't reach their ends.
Inputs may be any that keep to these rules, and one draw needn't show every extreme that they name: `selected`: each row names 64 different history blocks.
All inputs are finite; a program needn't handle non-finite values.
Results may differ from the reference program's by a relative error of at most 0.008.
The reference program's roundings to bfloat16 on the way count: a program that leaves them out, or rounds other values in their place, can miss the bound.
Values may be sent and summed in bfloat16 or wider, within the bound.
A program may use at most 128 MiB of HBM per device.

```python
import math
import jax
import jax.numpy as jnp
from jax import lax

D = 128
H = 4
HD = 32
CANDS = 512
BLOCK = 128
USERS = 16
HBLOCKS = 128
HIST = 16384
SEL = 64


def draw_candidates(key, part):
    base = jnp.clip(3.0 * jax.random.normal(key, (USERS, CANDS, D), jnp.float32), -18.0, 18.0)
    return base.astype(jnp.bfloat16)


def draw_history(key, part):
    base = jnp.clip(jax.random.normal(key, (USERS, HIST, D), jnp.float32), -6.0, 6.0)
    return base.astype(jnp.bfloat16)


def draw_selected(key, part):
    user_keys = jax.random.split(jax.random.fold_in(key, 3), USERS)
    orders = jax.vmap(lambda one_key: jax.random.permutation(one_key, HBLOCKS))(user_keys)
    return orders[:, :SEL].astype(jnp.int32)


def with_ends(entries, stream_key, smallest, high):
    index_at = [jax.random.randint(jax.random.fold_in(stream_key, axis), (), 0, length) for axis, length in enumerate(entries.shape)]
    longest = entries.shape.index(max(entries.shape))
    next_to = index_at[:longest] + [(index_at[longest] + 1) % entries.shape[longest]] + index_at[longest + 1:]
    return entries.at[tuple(index_at)].set(smallest).at[tuple(next_to)].set(high)


def level_of(own_key, dims, cuts, smallest, top_value):
    gain, own = 1.0, jax.random.fold_in(own_key, 6)
    for axis_at, blocks in cuts:
        steps = jnp.exp(jax.random.uniform(jax.random.fold_in(own, axis_at), (blocks,), jnp.float32, smallest / len(cuts), top_value / len(cuts)))
        gain = gain * jnp.repeat(steps, dims[axis_at] // blocks).reshape([-1 if axis == axis_at else 1 for axis in range(len(dims))])
    return gain


def gaussian(key, extent, deviation, bound, cuts=(), kind=jnp.bfloat16):
    drawn = jax.random.normal(key, extent, jnp.float32) * deviation
    if len(cuts) > 0:
        drawn = level_of(key, extent, cuts, -0.22, 0.18) * drawn
    return jnp.clip(drawn, min=-bound, max=bound).astype(kind)


def setup_inputs(seed: int = 0) -> dict:
    seeds = jax.random.split(jax.random.key(seed), 6)
    return {
        "candidates": draw_candidates(jax.random.fold_in(seeds[5], 71), 0),
        "history": draw_history(jax.random.fold_in(seeds[5], 71), 0),
        "projections": gaussian(seeds[2], (4, D, D), D ** -0.5, 0.5, ((1, 4),)),
        "lengths": with_ends(jax.random.randint(seeds[3], (USERS,), (HBLOCKS - SEL) * BLOCK + 1, HIST + 1), jax.random.fold_in(seeds[3], 1), (HBLOCKS - SEL) * BLOCK + 1, HIST).astype(jnp.int32),
        "selected": draw_selected(jax.random.fold_in(seeds[5], 71), 0),
    }


def reference(candidates, history, projections, lengths, selected):
    inv_root = 1.0 / math.sqrt(HD)
    offsets = jnp.arange(BLOCK, dtype=jnp.int32)

    def one_user(item):
        cand_rows, hist_rows, chosen, length = item
        queries = jnp.dot(cand_rows, projections[0], preferred_element_type=jnp.float32).astype(jnp.bfloat16)
        blocks = hist_rows.reshape(HBLOCKS, BLOCK, D)[chosen.astype(jnp.int32)].reshape(SEL * BLOCK, D)
        places = (chosen.astype(jnp.int32)[:, None] * BLOCK + offsets[None, :]).reshape(-1)
        live_keys = places < length
        keys = jnp.dot(blocks, projections[1], preferred_element_type=jnp.float32).astype(jnp.bfloat16)
        values = jnp.dot(blocks, projections[2], preferred_element_type=jnp.float32).astype(jnp.bfloat16)
        query_heads = queries.reshape(CANDS, H, HD).astype(jnp.float32)
        key_heads = keys.reshape(SEL * BLOCK, H, HD).astype(jnp.float32)
        value_heads = values.reshape(SEL * BLOCK, H, HD).astype(jnp.float32)
        scores = jnp.einsum('chd,khd->hck', query_heads, key_heads) * inv_root
        scores = jnp.where(live_keys[None, None, :], scores, -1e+30)
        maxima = lax.optimization_barrier(jnp.max(scores, axis=-1, keepdims=True))
        expo = jnp.where(live_keys[None, None, :], jnp.exp(scores - maxima), 0.0)
        totals = lax.optimization_barrier(jnp.sum(expo, axis=-1))
        rounded = lax.optimization_barrier(expo.astype(jnp.bfloat16)).astype(jnp.float32)
        summed = jnp.einsum('hck,khd->chd', rounded, value_heads)
        attended = (summed / totals.T[:, :, None]).reshape(CANDS, D).astype(jnp.bfloat16)
        return jnp.dot(attended, projections[3], preferred_element_type=jnp.float32).astype(jnp.bfloat16)
    return lax.map(one_user, (candidates, history, selected, lengths))
```

```python
import functools
import math

import jax
import jax.numpy as jnp
from jax import lax
from jax.experimental import pallas as pl
from jax.experimental.pallas import tpu as pltpu
from jax.sharding import PartitionSpec as P

H = 4
BLOCK = 128
PAIR = 2
TRIP = 2
PAD = 1 << 20
LOW = -1e30


def gather_kernel(
    n,
    ranks,
    lengths,
    cand,
    proj,
    hist,
    picks,
    all_cand,
    all_proj,
    all_keys,
    all_values,
    flags,
    rows_in,
    keys,
    values,
    own_sem,
    in_sem,
    out_sem,
    z_send,
    z_recv,
    y_send,
    y_recv,
    w_send,
    w_recv,
):
    mesh_id = pl.DeviceIdType.MESH
    me, rank = lax.axis_index("hist"), lax.axis_index("dp")
    line = n // 2
    side, spot = lax.rem(me, 2), me // 2
    users, own = cand.shape[0], cand.shape[1]
    rows = proj.shape[1]
    own_rows, embed = hist.shape[1], hist.shape[2]
    blocks = own_rows // BLOCK
    fetches = [pltpu.make_async_copy(hist.at[u], rows_in.at[u], in_sem.at[u]) for u in range(users)]
    for copy in fetches:
        copy.start()
    partner = spot * 2 + (1 - side)
    peers = [lax.rem(spot + k, line) * 2 + side for k in range(1, line)]
    mates = [lax.rem(rank + k, ranks) for k in range(1, ranks)]

    barrier = pltpu.get_barrier_semaphore()
    for peer in [partner] + peers:
        pl.semaphore_signal(barrier, inc=1, device_id={"hist": peer}, device_id_type=mesh_id)
    for mate in mates:
        pl.semaphore_signal(barrier, inc=1, device_id={"dp": mate}, device_id_type=mesh_id)
    pl.semaphore_wait(barrier, line + ranks - 1)

    def place(u, owner):
        return all_cand.at[u, pl.ds(pl.multiple_of(owner * own, own), own), :]

    strip = all_proj.at[:, pl.ds(pl.multiple_of(rank * rows, rows), rows), :]
    weight_copies = []
    for k, mate in enumerate(mates):
        copy = pltpu.make_async_remote_copy(
            proj, strip, w_send.at[k], w_recv.at[k], device_id={"dp": mate}, device_id_type=mesh_id
        )
        copy.start()
        weight_copies.append(copy)
    across, along = [], {}
    for u in range(users):
        for k, peer in enumerate(peers):
            copy = pltpu.make_async_remote_copy(
                cand.at[u],
                place(u, me),
                z_send.at[k, u],
                z_recv.at[k, u],
                device_id={"hist": peer},
                device_id_type=mesh_id,
            )
            copy.start()
            along[k, u] = copy
        copy = pltpu.make_async_remote_copy(
            cand.at[u],
            place(u, me),
            y_send.at[0, u],
            y_recv.at[0, u],
            device_id={"hist": partner},
            device_id_type=mesh_id,
        )
        copy.start()
        across.append(copy)
    locals_ = [pltpu.make_async_copy(proj, strip, own_sem.at[users])]
    locals_ += [pltpu.make_async_copy(cand.at[u], place(u, me), own_sem.at[u]) for u in range(users)]
    for copy in locals_:
        copy.start()
    spans = lax.broadcasted_iota(jnp.int32, (users, 128), 0)
    limits = jnp.zeros((users, 128), jnp.int32)
    for u in range(users):
        limits = jnp.where(spans == u, lengths[u], limits)
    lane = lax.broadcasted_iota(jnp.int32, (users, 128), 1)
    found = jnp.zeros((users, 128), jnp.int32)
    chosen = picks[...]
    for b in range(blocks):
        hit = jnp.max(jnp.where(chosen == me * blocks + b, 1.0, 0.0), axis=1, keepdims=True)
        found = jnp.where(jnp.logical_and(lane == b, hit > 0.0), 1, found)
    flags[...] = jnp.where((me * blocks + lane) * BLOCK < limits, found, 0)
    locals_[0].wait()
    for copy in weight_copies:
        copy.wait()
    key_weight, value_weight = all_proj[1], all_proj[2]
    shape = (blocks, BLOCK, embed)
    places = lax.broadcasted_iota(jnp.int32, shape, 0) * BLOCK + lax.broadcasted_iota(jnp.int32, shape, 1)
    places = places + me * own_rows
    stores = []
    for u in range(users):
        for k in range(line - 1):
            along[k, u].wait_recv()
            source = lax.rem(spot + line - (k + 1), line) * 2 + side
            copy = pltpu.make_async_remote_copy(
                place(u, source),
                place(u, source),
                y_send.at[k + 1, u],
                y_recv.at[k + 1, u],
                device_id={"hist": partner},
                device_id_type=mesh_id,
            )
            copy.start()
            across.append(copy)
        fetches[u].wait()
        block_rows = rows_in[u].reshape(shape).astype(jnp.float32)
        alive = places < lengths[u]
        safe = jnp.where(alive, block_rows, block_rows[:, 0:1, :]).astype(jnp.bfloat16).reshape(own_rows, embed)
        kept = jnp.where(alive, block_rows, 0.0).astype(jnp.bfloat16).reshape(own_rows, embed)
        keys[u] = jnp.dot(safe, key_weight, preferred_element_type=jnp.float32).astype(jnp.bfloat16)
        values[u] = lax.dot_general(
            value_weight, kept, (((0,), (1,)), ((), ())), preferred_element_type=jnp.float32
        ).astype(jnp.bfloat16)
        for k, (src, dst) in enumerate(((keys, all_keys), (values, all_values))):
            copy = pltpu.make_async_copy(src.at[u], dst.at[u], out_sem.at[k, u])
            copy.start()
            stores.append(copy)
    for copy in along.values():
        copy.wait_send()
    for copy in across + locals_[1:] + stores:
        copy.wait()


def attend_kernel(
    own_cands,
    lengths,
    flags,
    base,
    cand,
    keys,
    values,
    weights,
    parts,
    stats,
    qpad,
    acc,
    top,
    scores,
    peaks,
    probs,
    shrinks,
    slots,
    owners,
):
    users, cands, embed = cand.shape
    head = embed // H
    tall = acc[0].shape[1]
    blocks = keys.shape[1] // BLOCK
    factor = math.log2(math.e) / math.sqrt(head)
    first = base[0]

    owners[0] = 0
    slots[0] = PAD
    slots[1] = PAD
    item = jnp.int32(1)
    for u in range(users):
        last = jnp.int32(0)
        at = item * PAIR
        for b in range(blocks):
            alive = flags[u, b]
            slots[at] = b
            at = at + alive
            last = jnp.where(alive > 0, b, last)
        for k in range(3 * PAIR):
            slots[at + k] = last + PAD
        for p in range(blocks // PAIR + 3):
            owners[item + p] = u
        item = (at + 1) // PAIR

    for u in range(users):
        query = lax.dot_general(
            weights[0], cand[u], (((0,), (1,)), ((), ())), preferred_element_type=jnp.float32
        ).astype(jnp.bfloat16)
        for h in range(H):
            rows = slice(h * head, (h + 1) * head)
            pieces = []
            if h > 0:
                pieces.append(jnp.zeros((h * head, cands), jnp.bfloat16))
            pieces.append(query[rows, :])
            if h < H - 1:
                pieces.append(jnp.zeros((embed - (h + 1) * head, cands), jnp.bfloat16))
            qpad[h][u] = jnp.concatenate(pieces, axis=0)
    for h in range(H):
        acc[h][...] = jnp.zeros(acc[h].shape, jnp.float32)
        top[h][...] = jnp.full(top[h].shape, LOW, jnp.float32)
    probs[1][...] = jnp.zeros(probs[1].shape, jnp.bfloat16)
    shrinks[1][...] = jnp.ones(shrinks[1].shape, jnp.float32)

    right = lax.broadcasted_iota(jnp.int32, (tall - head, BLOCK), 1)
    under = lax.broadcasted_iota(jnp.int32, (tall - head, BLOCK), 0)
    right = jnp.where(under == 0, right, jnp.iinfo(jnp.int32).max)

    def start_of(slot):
        block = jnp.where(slot >= PAD, slot - PAD, slot)
        return pl.multiple_of(block * BLOCK, BLOCK)

    def load_scores(i, h, buf):
        user = owners[i]
        key = jnp.concatenate([keys[user, pl.ds(start_of(slots[i * PAIR + k]), BLOCK), :] for k in range(PAIR)], axis=0)
        got = jnp.dot(key, qpad[h][user], preferred_element_type=jnp.float32)
        scores[buf][...] = got
        peaks[buf][...] = jnp.max(got, axis=0, keepdims=True)

    def weigh(i, h, buf):
        user = owners[i]
        before = top[h][user]
        peak = jnp.maximum(before, peaks[buf][...])
        probs[buf][...] = jnp.exp2((scores[buf][...] - peak) * factor).astype(jnp.bfloat16)
        shrinks[buf][...] = jnp.exp2((before - peak) * factor)
        top[h][user] = peak

    def gain(i, h, buf):
        user = owners[i]
        pieces = []
        for k in range(PAIR):
            slot = slots[i * PAIR + k]
            start = start_of(slot)
            limit = jnp.where(slot >= PAD, 0, lengths[user] - (start + first * BLOCK))
            one = jnp.where(right < limit, 1.0, 0.0).astype(jnp.bfloat16)
            value = values[user, h * head : (h + 1) * head, pl.ds(start, BLOCK)]
            value = jnp.where(slot >= PAD, jnp.zeros_like(value), value)
            pieces.append(jnp.concatenate([value, one], axis=0))
        value = jnp.concatenate(pieces, axis=1)
        acc[h][user] = acc[h][user] * shrinks[buf][...] + jnp.dot(
            value, probs[buf][...], preferred_element_type=jnp.float32
        )

    load_scores(1, 0, 0)

    @pl.loop(0, (item - 1 + TRIP - 1) // TRIP)
    def _(step):
        begin = step * TRIP + 1
        for s in range(TRIP * H):
            buf = s % 2
            load_scores(begin + (s + 1) // H, (s + 1) % H, 1 - buf)
            gain(begin + (s + H - 1) // H - 1, (s + H - 1) % H, 1 - buf)
            weigh(begin + s // H, s % H, buf)

    gain((item - 1 + TRIP - 1) // TRIP * TRIP, H - 1, 1)

    means, logs = [], []
    for u in range(users):
        rows, row_logs = [], []
        for h in range(H):
            amount = acc[h][u, head : head + 1, :]
            some = amount > 0.0
            safe = jnp.where(some, amount, 1.0)
            rows.append((acc[h][u, 0:head, :] * (1.0 / safe)).astype(jnp.bfloat16))
            row_logs.append(jnp.where(some, top[h][u] * factor + jnp.log2(safe), LOW))
        means.append(jnp.concatenate(rows, axis=0))
        logs.append(jnp.concatenate(row_logs, axis=0))
    for dest in range(parts.shape[0]):
        at = slice(dest * own_cands, (dest + 1) * own_cands)
        to = slice(0, users * own_cands)
        parts[dest, :, to] = jnp.concatenate([m[:, at] for m in means], axis=1)
        stats[dest, :, to] = jnp.concatenate([m[:, at] for m in logs], axis=1)


def combine_kernel(n, parts, stats, out_weight, result, got, got_stats, send_a, recv_a, send_b, recv_b):
    me = lax.axis_index("hist")
    barrier = pltpu.get_barrier_semaphore()
    for k in range(1, n):
        pl.semaphore_signal(
            barrier, inc=1, device_id={"hist": lax.rem(me + k, n)}, device_id_type=pl.DeviceIdType.MESH
        )
    pl.semaphore_wait(barrier, n - 1)
    copies = []
    for k in range(1, n):
        peer = lax.rem(me + k, n)
        for src, dst, send, recv in ((stats, got_stats, send_b, recv_b), (parts, got, send_a, recv_a)):
            copy = pltpu.make_async_remote_copy(
                src_ref=src.at[peer],
                dst_ref=dst.at[k - 1],
                send_sem=send.at[k - 1],
                recv_sem=recv.at[k - 1],
                device_id={"hist": peer},
                device_id_type=pl.DeviceIdType.MESH,
            )
            copy.start()
            copies.append(copy)
    for copy in copies:
        copy.wait()
    logs = [stats[me]] + [got_stats[k] for k in range(n - 1)]
    highest = functools.reduce(jnp.maximum, logs)
    shares = [jnp.exp2(log - highest) for log in logs]
    inverse = 1.0 / functools.reduce(jnp.add, shares)
    embed = parts.shape[1]
    head = embed // H
    pieces = []
    for h in range(H):
        rows = slice(h * head, (h + 1) * head)
        mixed = parts[me, rows, :].astype(jnp.float32) * shares[0][h : h + 1, :]
        for k in range(n - 1):
            mixed += got[k, rows, :].astype(jnp.float32) * shares[k + 1][h : h + 1, :]
        pieces.append(mixed * inverse[h : h + 1, :])
    attended = jnp.concatenate(pieces, axis=0).astype(jnp.bfloat16)
    result[...] = lax.dot_general(
        attended, out_weight[3], (((0,), (0,)), ((), ())), preferred_element_type=jnp.float32
    ).astype(jnp.bfloat16)


def body(candidates, history, projections, lengths, selected):
    n = lax.axis_size("hist")
    ranks = lax.axis_size("dp")
    users, own_cands, embed = candidates.shape
    cands = n * own_cands
    line = n // 2
    own_rows = history.shape[1]
    blocks = own_rows // BLOCK
    first = (lax.axis_index("hist") * blocks).astype(jnp.int32)
    base = first.reshape(1)
    whole, weights, keys, values, flags = pl.pallas_call(
        functools.partial(gather_kernel, n, ranks),
        out_shape=[
            jax.ShapeDtypeStruct((users, cands, embed), jnp.bfloat16),
            jax.ShapeDtypeStruct((projections.shape[0], ranks * projections.shape[1], embed), jnp.bfloat16),
            jax.ShapeDtypeStruct((users, own_rows, embed), jnp.bfloat16),
            jax.ShapeDtypeStruct((users, embed, own_rows), jnp.bfloat16),
            jax.ShapeDtypeStruct((users, 128), jnp.int32),
        ],
        in_specs=[pl.BlockSpec(memory_space=pltpu.SMEM)]
        + [pl.BlockSpec(memory_space=pltpu.VMEM)] * 2
        + [pl.BlockSpec(memory_space=pl.ANY), pl.BlockSpec(memory_space=pltpu.VMEM)],
        out_specs=[pl.BlockSpec(memory_space=pltpu.VMEM)] * 2
        + [pl.BlockSpec(memory_space=pl.ANY)] * 2
        + [pl.BlockSpec(memory_space=pltpu.VMEM)],
        scratch_shapes=[
            pltpu.VMEM((users, own_rows, embed), jnp.bfloat16),
            pltpu.VMEM((users, own_rows, embed), jnp.bfloat16),
            pltpu.VMEM((users, embed, own_rows), jnp.bfloat16),
            pltpu.SemaphoreType.DMA((users + 1,)),
            pltpu.SemaphoreType.DMA((users,)),
            pltpu.SemaphoreType.DMA((2, users)),
            pltpu.SemaphoreType.DMA((line - 1, users)),
            pltpu.SemaphoreType.DMA((line - 1, users)),
            pltpu.SemaphoreType.DMA((line, users)),
            pltpu.SemaphoreType.DMA((line, users)),
            pltpu.SemaphoreType.DMA((ranks - 1,)),
            pltpu.SemaphoreType.DMA((ranks - 1,)),
        ],
        compiler_params=pltpu.CompilerParams(collective_id=1, has_side_effects=True),
        name="gather",
    )(lengths, candidates, projections, history, selected)
    wide = -(-users * own_cands // 128) * 128
    parts, stats = pl.pallas_call(
        functools.partial(attend_kernel, own_cands),
        in_specs=[pl.BlockSpec(memory_space=pltpu.SMEM)] * 3 + [pl.BlockSpec(memory_space=pltpu.VMEM)] * 4,
        out_specs=[pl.BlockSpec(memory_space=pltpu.VMEM)] * 2,
        scratch_shapes=[
            [pltpu.VMEM((users, embed, cands), jnp.bfloat16)] * H,
            [pltpu.VMEM((users, embed // H + 16, cands), jnp.float32)] * H,
            [pltpu.VMEM((users, 1, cands), jnp.float32)] * H,
            [pltpu.VMEM((PAIR * BLOCK, cands), jnp.float32)] * 2,
            [pltpu.VMEM((1, cands), jnp.float32)] * 2,
            [pltpu.VMEM((PAIR * BLOCK, cands), jnp.bfloat16)] * 2,
            [pltpu.VMEM((1, cands), jnp.float32)] * 2,
            pltpu.SMEM(((users * blocks) + users * PAIR + 8 * PAIR,), jnp.int32),
            pltpu.SMEM((users * (blocks // PAIR + 1) + 8,), jnp.int32),
        ],
        out_shape=[
            jax.ShapeDtypeStruct((n, embed, wide), jnp.bfloat16),
            jax.ShapeDtypeStruct((n, H, wide), jnp.float32),
        ],
        name="attend",
    )(lengths, flags, base, whole, keys, values, weights)
    result = pl.pallas_call(
        functools.partial(combine_kernel, n),
        out_shape=jax.ShapeDtypeStruct((wide, embed), jnp.bfloat16),
        in_specs=[pl.BlockSpec(memory_space=pltpu.VMEM)] * 3,
        out_specs=pl.BlockSpec(memory_space=pltpu.VMEM),
        scratch_shapes=[
            pltpu.VMEM((n - 1, embed, wide), jnp.bfloat16),
            pltpu.VMEM((n - 1, H, wide), jnp.float32),
        ]
        + [pltpu.SemaphoreType.DMA((n - 1,))] * 4,
        compiler_params=pltpu.CompilerParams(collective_id=0, has_side_effects=True),
        name="combine",
    )(parts, stats, weights)
    return result[: users * own_cands].reshape(users, own_cands, embed)


def solution(mesh):
    placed = (
        P("dp", "hist", None),
        P("dp", "hist", None),
        P(None, "dp", None),
        P("dp"),
        P("dp", None),
    )
    return jax.shard_map(
        body, mesh=mesh, in_specs=placed, out_specs=P("dp", "hist", None), check_vma=False
    )
```

```python
import functools
import math

import jax
import jax.numpy as jnp
from jax import lax
from jax.experimental import pallas as pl
from jax.experimental.pallas import tpu as pltpu
from jax.sharding import PartitionSpec as P

H = 4
BLOCK = 128
PAIR = 2
TRIP = 2
PAD = 1 << 20
LAG = 2
SAMPLE = 32
SMALL = 2.0**-30
LARGE = 2.0**100
ROOM = 40 << 20
LOW = -1e30


def gather_kernel(
    n,
    ranks,
    lengths,
    cand,
    proj,
    hist,
    picks,
    all_cand,
    all_proj,
    keys,
    values,
    flags,
    rows_in,
    own_sem,
    in_sem,
    z_send,
    z_recv,
    y_send,
    y_recv,
    w_send,
    w_recv,
):
    mesh_id = pl.DeviceIdType.MESH
    me, rank = lax.axis_index("hist"), lax.axis_index("dp")
    line = n // 2
    side, spot = lax.rem(me, 2), me // 2
    users, own = cand.shape[0], cand.shape[1]
    rows = proj.shape[1]
    own_rows, embed = hist.shape[1], hist.shape[2]
    blocks = own_rows // BLOCK
    fetches = [pltpu.make_async_copy(hist.at[u], rows_in.at[u], in_sem.at[u]) for u in range(users)]
    for copy in fetches:
        copy.start()
    partner = spot * 2 + (1 - side)
    peers = [lax.rem(spot + k, line) * 2 + side for k in range(1, line)]
    mates = [lax.rem(rank + k, ranks) for k in range(1, ranks)]

    barrier = pltpu.get_barrier_semaphore()
    for peer in [partner] + peers:
        pl.semaphore_signal(barrier, inc=1, device_id={"hist": peer}, device_id_type=mesh_id)
    for mate in mates:
        pl.semaphore_signal(barrier, inc=1, device_id={"dp": mate}, device_id_type=mesh_id)
    pl.semaphore_wait(barrier, line + ranks - 1)

    def place(u, owner):
        return all_cand.at[u, pl.ds(pl.multiple_of(owner * own, own), own), :]

    strip = all_proj.at[:, pl.ds(pl.multiple_of(rank * rows, rows), rows), :]
    weight_copies = []
    for k, mate in enumerate(mates):
        copy = pltpu.make_async_remote_copy(
            proj, strip, w_send.at[k], w_recv.at[k], device_id={"dp": mate}, device_id_type=mesh_id
        )
        copy.start()
        weight_copies.append(copy)
    across, along = [], {}
    for u in range(users):
        for k, peer in enumerate(peers):
            copy = pltpu.make_async_remote_copy(
                cand.at[u],
                place(u, me),
                z_send.at[k, u],
                z_recv.at[k, u],
                device_id={"hist": peer},
                device_id_type=mesh_id,
            )
            copy.start()
            along[k, u] = copy
        copy = pltpu.make_async_remote_copy(
            cand.at[u],
            place(u, me),
            y_send.at[0, u],
            y_recv.at[0, u],
            device_id={"hist": partner},
            device_id_type=mesh_id,
        )
        copy.start()
        across.append(copy)
    locals_ = [pltpu.make_async_copy(proj, strip, own_sem.at[users])]
    locals_ += [pltpu.make_async_copy(cand.at[u], place(u, me), own_sem.at[u]) for u in range(users)]
    for copy in locals_:
        copy.start()
    spans = lax.broadcasted_iota(jnp.int32, (users, 128), 0)
    limits = jnp.zeros((users, 128), jnp.int32)
    for u in range(users):
        limits = jnp.where(spans == u, lengths[u], limits)
    lane = lax.broadcasted_iota(jnp.int32, (users, 128), 1)
    found = jnp.zeros((users, 128), jnp.int32)
    chosen = picks[...]
    for b in range(blocks):
        hit = jnp.max(jnp.where(chosen == me * blocks + b, 1.0, 0.0), axis=1, keepdims=True)
        found = jnp.where(jnp.logical_and(lane == b, hit > 0.0), 1, found)
    flags[...] = jnp.where((me * blocks + lane) * BLOCK < limits, found, 0)
    locals_[0].wait()
    for copy in weight_copies:
        copy.wait()
    key_weight, value_weight = all_proj[1], all_proj[2]
    shape = (blocks, BLOCK, embed)
    places = lax.broadcasted_iota(jnp.int32, shape, 0) * BLOCK + lax.broadcasted_iota(jnp.int32, shape, 1)
    places = places + me * own_rows
    for u in range(users):
        for k in range(line - 1):
            along[k, u].wait_recv()
            source = lax.rem(spot + line - (k + 1), line) * 2 + side
            copy = pltpu.make_async_remote_copy(
                place(u, source),
                place(u, source),
                y_send.at[k + 1, u],
                y_recv.at[k + 1, u],
                device_id={"hist": partner},
                device_id_type=mesh_id,
            )
            copy.start()
            across.append(copy)
        fetches[u].wait()
        block_rows = rows_in[u].reshape(shape).astype(jnp.float32)
        alive = places < lengths[u]
        safe = jnp.where(alive, block_rows, block_rows[:, 0:1, :]).astype(jnp.bfloat16).reshape(own_rows, embed)
        kept = jnp.where(alive, block_rows, 0.0).astype(jnp.bfloat16).reshape(own_rows, embed)
        keys[u] = jnp.dot(safe, key_weight, preferred_element_type=jnp.float32).astype(jnp.bfloat16)
        values[u] = lax.dot_general(
            value_weight, kept, (((0,), (1,)), ((), ())), preferred_element_type=jnp.float32
        ).astype(jnp.bfloat16)
    for copy in along.values():
        copy.wait_send()
    for copy in across + locals_[1:]:
        copy.wait()


def attend_kernel(
    own_cands,
    lengths,
    flags,
    base,
    cand,
    keys,
    values,
    weights,
    parts,
    stats,
    query,
    acc,
    shift,
    top,
    probs,
    slots,
    owners,
):
    users, cands, embed = cand.shape
    head = embed // H
    half = embed // 2
    tall = acc[0].shape[1]
    blocks = keys.shape[1] // BLOCK
    factor = math.log2(math.e) / math.sqrt(head)
    first = base[0]

    owners[0] = 0
    slots[0] = PAD
    slots[1] = PAD
    item = jnp.int32(1)
    begins, counts = [], []
    for u in range(users):
        last = jnp.int32(0)
        at = item * PAIR
        begins.append(item)
        for b in range(blocks):
            alive = flags[u, b]
            slots[at] = b
            at = at + alive
            last = jnp.where(alive > 0, b, last)
        for k in range(3 * PAIR):
            slots[at + k] = last + PAD
        for p in range(blocks // PAIR + 3):
            owners[item + p] = u
        counts.append(at - item * PAIR)
        item = (at + 1) // PAIR
    trips = (item - 1 + TRIP - 1) // TRIP

    def start_of(slot):
        block = jnp.where(slot >= PAD, slot - PAD, slot)
        return pl.multiple_of(block * BLOCK, BLOCK)

    column = lax.broadcasted_iota(jnp.int32, (1, embed), 1)
    group = [(h * head) // half for h in range(H)]
    spot = [(1 - group[h]) * half + (h - group[h] * (H // 2)) * 16 for h in range(H)]
    mine = [jnp.where(column // head == h, 1.0, 0.0).astype(jnp.bfloat16) for h in range(H)]
    mark = [jnp.where(column == spot[h], 1.0, 0.0).astype(jnp.bfloat16) for h in range(H)]
    lead = lax.broadcasted_iota(jnp.int32, (16, cands), 0) == 0

    for u in range(users):
        plain = lax.dot_general(
            weights[0], cand[u], (((0,), (1,)), ((), ())), preferred_element_type=jnp.float32
        ).astype(jnp.bfloat16)
        scaled = plain.astype(jnp.float32) * factor
        high = scaled.astype(jnp.bfloat16)
        low = (scaled - high.astype(jnp.float32)).astype(jnp.bfloat16)
        for g in range(2):
            query[g][u, 0:embed, :] = high
            query[g][u, embed : 2 * embed, :] = low
        sample = keys[u, pl.ds(start_of(slots[begins[u] * PAIR]), SAMPLE), :]
        guess = jnp.dot(
            jnp.concatenate([sample * mine[h] for h in range(H)], axis=0), high, preferred_element_type=jnp.float32
        )
        for h in range(H):
            most = jnp.max(guess[h * SAMPLE : (h + 1) * SAMPLE, :], axis=0, keepdims=True)
            most = most.astype(jnp.bfloat16).astype(jnp.float32)
            shift[h][u] = most
            query[group[h]][u, embed + spot[h] : embed + spot[h] + 16, :] = jnp.where(lead, -most, 0.0).astype(
                jnp.bfloat16
            )
    for h in range(H):
        acc[h][...] = jnp.zeros(acc[h].shape, jnp.float32)
    for k in range(2):
        probs[2 + k][...] = jnp.zeros(probs[2 + k].shape, jnp.bfloat16)

    right = lax.broadcasted_iota(jnp.int32, (tall - head, BLOCK), 1)
    under = lax.broadcasted_iota(jnp.int32, (tall - head, BLOCK), 0)
    right = jnp.where(under == 0, right, jnp.iinfo(jnp.int32).max)

    def scores(i, h):
        user = owners[i]
        key = jnp.concatenate([keys[user, pl.ds(start_of(slots[i * PAIR + k]), BLOCK), :] for k in range(PAIR)], axis=0)
        key = key * mine[h]
        return jnp.dot(
            jnp.concatenate([key, key + mark[h]], axis=1), query[group[h]][user], preferred_element_type=jnp.float32
        )

    def gain(i, h, prob):
        user = owners[i]
        pieces = []
        for k in range(PAIR):
            slot = slots[i * PAIR + k]
            start = start_of(slot)
            limit = jnp.where(slot >= PAD, 0, lengths[user] - (start + first * BLOCK))
            one = jnp.where(right < limit, 1.0, 0.0).astype(jnp.bfloat16)
            value = values[user, h * head : (h + 1) * head, pl.ds(start, BLOCK)]
            value = jnp.where(slot >= PAD, jnp.zeros_like(value), value)
            pieces.append(jnp.concatenate([value, one], axis=0))
        return jnp.dot(jnp.concatenate(pieces, axis=1), prob, preferred_element_type=jnp.float32)

    @pl.loop(0, trips)
    def _(step):
        begin = step * TRIP + 1
        for s in range(TRIP * H):
            late, head_late = begin + (s + 2 * H - LAG) // H - 2, (s + H - LAG) % H
            probs[s % 4][...] = jnp.exp2(scores(begin + s // H, s % H)).astype(jnp.bfloat16)
            acc[head_late][owners[late]] += gain(late, head_late, probs[(s - LAG) % 4][...])

    for k in range(LAG):
        h = H - LAG + k
        user = owners[trips * TRIP]
        acc[h][user] += gain(trips * TRIP, h, probs[(TRIP * H - LAG + k) % 4][...])

    wrong = jnp.zeros((1, cands), jnp.float32)
    for u in range(users):
        for h in range(H):
            amount = acc[h][u, head : head + 1, :]
            fine = jnp.logical_and(amount > SMALL, amount < LARGE)
            wrong = jnp.maximum(wrong, jnp.where(fine, 0.0, jnp.where(counts[u] > 0, 1.0, 0.0)))

    @pl.when(jnp.max(wrong) > 0.0)
    def _():
        for h in range(H):
            acc[h][...] = jnp.zeros(acc[h].shape, jnp.float32)
            top[h][...] = jnp.full(top[h].shape, LOW, jnp.float32)

        @pl.loop(1, item)
        def _(i):
            user = owners[i]
            for h in range(H):
                got = scores(i, h)
                before = top[h][user]
                peak = jnp.maximum(before, jnp.max(got, axis=0, keepdims=True))
                prob = jnp.exp2(got - peak).astype(jnp.bfloat16)
                acc[h][user] = acc[h][user] * jnp.exp2(before - peak) + gain(i, h, prob)
                top[h][user] = peak

        for h in range(H):
            shift[h][...] = shift[h][...] + top[h][...]

    means, logs = [], []
    for u in range(users):
        rows, row_logs = [], []
        for h in range(H):
            amount = acc[h][u, head : head + 1, :]
            some = jnp.logical_and(counts[u] > 0, amount > 0.0)
            safe = jnp.where(some, amount, 1.0)
            mean = jnp.where(some, acc[h][u, 0:head, :] * (1.0 / safe), 0.0)
            rows.append(mean.astype(jnp.bfloat16))
            row_logs.append(jnp.where(some, shift[h][u] + jnp.log2(safe), LOW))
        means.append(jnp.concatenate(rows, axis=0))
        logs.append(jnp.concatenate(row_logs, axis=0))
    for dest in range(parts.shape[0]):
        at = slice(dest * own_cands, (dest + 1) * own_cands)
        to = slice(0, users * own_cands)
        parts[dest, :, to] = jnp.concatenate([m[:, at] for m in means], axis=1)
        stats[dest, :, to] = jnp.concatenate([m[:, at] for m in logs], axis=1)


def combine_kernel(n, parts, stats, out_weight, result, got, got_stats, send_a, recv_a, send_b, recv_b):
    me = lax.axis_index("hist")
    barrier = pltpu.get_barrier_semaphore()
    for k in range(1, n):
        pl.semaphore_signal(
            barrier, inc=1, device_id={"hist": lax.rem(me + k, n)}, device_id_type=pl.DeviceIdType.MESH
        )
    pl.semaphore_wait(barrier, n - 1)
    copies = []
    for k in range(1, n):
        peer = lax.rem(me + k, n)
        for src, dst, send, recv in ((stats, got_stats, send_b, recv_b), (parts, got, send_a, recv_a)):
            copy = pltpu.make_async_remote_copy(
                src_ref=src.at[peer],
                dst_ref=dst.at[k - 1],
                send_sem=send.at[k - 1],
                recv_sem=recv.at[k - 1],
                device_id={"hist": peer},
                device_id_type=pl.DeviceIdType.MESH,
            )
            copy.start()
            copies.append(copy)
    for copy in copies:
        copy.wait()
    logs = [stats[me]] + [got_stats[k] for k in range(n - 1)]
    highest = functools.reduce(jnp.maximum, logs)
    shares = [jnp.exp2(log - highest) for log in logs]
    inverse = 1.0 / functools.reduce(jnp.add, shares)
    embed = parts.shape[1]
    head = embed // H
    pieces = []
    for h in range(H):
        rows = slice(h * head, (h + 1) * head)
        mixed = parts[me, rows, :].astype(jnp.float32) * shares[0][h : h + 1, :]
        for k in range(n - 1):
            mixed += got[k, rows, :].astype(jnp.float32) * shares[k + 1][h : h + 1, :]
        pieces.append(mixed * inverse[h : h + 1, :])
    attended = jnp.concatenate(pieces, axis=0).astype(jnp.bfloat16)
    result[...] = lax.dot_general(
        attended, out_weight[3], (((0,), (0,)), ((), ())), preferred_element_type=jnp.float32
    ).astype(jnp.bfloat16)


def body(candidates, history, projections, lengths, selected):
    n = lax.axis_size("hist")
    ranks = lax.axis_size("dp")
    users, own_cands, embed = candidates.shape
    cands = n * own_cands
    line = n // 2
    own_rows = history.shape[1]
    blocks = own_rows // BLOCK
    first = (lax.axis_index("hist") * blocks).astype(jnp.int32)
    base = first.reshape(1)
    whole, weights, keys, values, flags = pl.pallas_call(
        functools.partial(gather_kernel, n, ranks),
        out_shape=[
            pltpu.VMEM((users, cands, embed), jnp.bfloat16),
            pltpu.VMEM((projections.shape[0], ranks * projections.shape[1], embed), jnp.bfloat16),
            pltpu.VMEM((users, own_rows, embed), jnp.bfloat16),
            pltpu.VMEM((users, embed, own_rows), jnp.bfloat16),
            jax.ShapeDtypeStruct((users, 128), jnp.int32),
        ],
        in_specs=[pl.BlockSpec(memory_space=pltpu.SMEM)]
        + [pl.BlockSpec(memory_space=pltpu.VMEM)] * 2
        + [pl.BlockSpec(memory_space=pl.ANY), pl.BlockSpec(memory_space=pltpu.VMEM)],
        out_specs=[pl.BlockSpec(memory_space=pltpu.VMEM)] * 5,
        scratch_shapes=[
            pltpu.VMEM((users, own_rows, embed), jnp.bfloat16),
            pltpu.SemaphoreType.DMA((users + 1,)),
            pltpu.SemaphoreType.DMA((users,)),
            pltpu.SemaphoreType.DMA((line - 1, users)),
            pltpu.SemaphoreType.DMA((line - 1, users)),
            pltpu.SemaphoreType.DMA((line, users)),
            pltpu.SemaphoreType.DMA((line, users)),
            pltpu.SemaphoreType.DMA((ranks - 1,)),
            pltpu.SemaphoreType.DMA((ranks - 1,)),
        ],
        compiler_params=pltpu.CompilerParams(collective_id=1, has_side_effects=True, vmem_limit_bytes=ROOM),
        name="gather",
    )(lengths, candidates, projections, history, selected)
    wide = -(-users * own_cands // 128) * 128
    parts, stats = pl.pallas_call(
        functools.partial(attend_kernel, own_cands),
        in_specs=[pl.BlockSpec(memory_space=pltpu.SMEM)] * 3 + [pl.BlockSpec(memory_space=pltpu.VMEM)] * 4,
        out_specs=[pl.BlockSpec(memory_space=pltpu.VMEM)] * 2,
        scratch_shapes=[
            [pltpu.VMEM((users, 2 * embed, cands), jnp.bfloat16)] * 2,
            [pltpu.VMEM((users, embed // H + 16, cands), jnp.float32)] * H,
            [pltpu.VMEM((users, 1, cands), jnp.float32)] * H,
            [pltpu.VMEM((users, 1, cands), jnp.float32)] * H,
            [pltpu.VMEM((PAIR * BLOCK, cands), jnp.bfloat16)] * 4,
            pltpu.SMEM(((users * blocks) + users * PAIR + 8 * PAIR,), jnp.int32),
            pltpu.SMEM((users * (blocks // PAIR + 1) + 8,), jnp.int32),
        ],
        out_shape=[
            pltpu.VMEM((n, embed, wide), jnp.bfloat16),
            pltpu.VMEM((n, H, wide), jnp.float32),
        ],
        compiler_params=pltpu.CompilerParams(vmem_limit_bytes=ROOM),
        name="attend",
    )(lengths, flags, base, whole, keys, values, weights)
    result = pl.pallas_call(
        functools.partial(combine_kernel, n),
        out_shape=jax.ShapeDtypeStruct((wide, embed), jnp.bfloat16),
        in_specs=[pl.BlockSpec(memory_space=pltpu.VMEM)] * 3,
        out_specs=pl.BlockSpec(memory_space=pltpu.VMEM),
        scratch_shapes=[
            pltpu.VMEM((n - 1, embed, wide), jnp.bfloat16),
            pltpu.VMEM((n - 1, H, wide), jnp.float32),
        ]
        + [pltpu.SemaphoreType.DMA((n - 1,))] * 4,
        compiler_params=pltpu.CompilerParams(collective_id=0, has_side_effects=True, vmem_limit_bytes=ROOM),
        name="combine",
    )(parts, stats, weights)
    return result[: users * own_cands].reshape(users, own_cands, embed)


def solution(mesh):
    placed = (
        P("dp", "hist", None),
        P("dp", "hist", None),
        P(None, "dp", None),
        P("dp"),
        P("dp", None),
    )
    return jax.shard_map(
        body, mesh=mesh, in_specs=placed, out_specs=P("dp", "hist", None), check_vma=False
    )
```

```python
import functools
import math

import jax
import jax.numpy as jnp
from jax import lax
from jax.experimental import pallas as pl
from jax.experimental.pallas import tpu as pltpu
from jax.sharding import PartitionSpec as P

H = 4
BLOCK = 128
PAIR = 2
TRIP = 2
PAD = 1 << 20
LAG = 2
SAMPLE = 32
SMALL = 2.0**-30
LARGE = 2.0**100
ROOM = 40 << 20
LOW = -1e30


def gather_kernel(
    n,
    ranks,
    lengths,
    cand_in,
    proj_in,
    hist,
    picks_in,
    all_proj,
    high,
    low,
    keys,
    values,
    flags,
    cand,
    proj,
    picks,
    all_cand,
    rows_in,
    own_sem,
    arg_sem,
    in_sem,
    z_send,
    z_recv,
    y_send,
    y_recv,
    w_send,
    w_recv,
):
    mesh_id = pl.DeviceIdType.MESH
    me, rank = lax.axis_index("hist"), lax.axis_index("dp")
    line = n // 2
    side, spot = lax.rem(me, 2), me // 2
    users, own = cand.shape[0], cand.shape[1]
    rows = proj.shape[1]
    own_rows, embed = hist.shape[1], hist.shape[2]
    blocks = own_rows // BLOCK
    factor = math.log2(math.e) / math.sqrt(embed // H)

    def place(u, owner):
        return all_cand.at[u, pl.ds(pl.multiple_of(owner * own, own), own), :]

    loads = [
        pltpu.make_async_copy(src, dst, arg_sem.at[k])
        for k, (src, dst) in enumerate(((proj_in, proj), (cand_in, cand), (picks_in, picks)))
    ]
    strip = all_proj.at[:, pl.ds(pl.multiple_of(rank * rows, rows), rows), :]
    locals_ = [pltpu.make_async_copy(proj_in, strip, own_sem.at[users])]
    locals_ += [pltpu.make_async_copy(cand_in.at[u], place(u, me), own_sem.at[u]) for u in range(users)]
    fetches = [pltpu.make_async_copy(hist.at[u], rows_in.at[u], in_sem.at[u]) for u in range(users)]
    for copy in loads + locals_ + fetches:
        copy.start()
    partner = spot * 2 + (1 - side)
    peers = [lax.rem(spot + k, line) * 2 + side for k in range(1, line)]
    mates = [lax.rem(rank + k, ranks) for k in range(1, ranks)]

    barrier = pltpu.get_barrier_semaphore()
    for peer in [partner] + peers:
        pl.semaphore_signal(barrier, inc=1, device_id={"hist": peer}, device_id_type=mesh_id)
    for mate in mates:
        pl.semaphore_signal(barrier, inc=1, device_id={"dp": mate}, device_id_type=mesh_id)
    pl.semaphore_wait(barrier, line + ranks - 1)

    loads[0].wait()
    loads[1].wait()
    weight_copies = []
    for k, mate in enumerate(mates):
        copy = pltpu.make_async_remote_copy(
            proj, strip, w_send.at[k], w_recv.at[k], device_id={"dp": mate}, device_id_type=mesh_id
        )
        copy.start()
        weight_copies.append(copy)
    across, along = {}, {}
    for u in range(users):
        for k, peer in enumerate(peers):
            copy = pltpu.make_async_remote_copy(
                cand.at[u],
                place(u, me),
                z_send.at[k, u],
                z_recv.at[k, u],
                device_id={"hist": peer},
                device_id_type=mesh_id,
            )
            copy.start()
            along[k, u] = copy
        copy = pltpu.make_async_remote_copy(
            cand.at[u],
            place(u, me),
            y_send.at[0, u],
            y_recv.at[0, u],
            device_id={"hist": partner},
            device_id_type=mesh_id,
        )
        copy.start()
        across[0, u] = copy
    loads[2].wait()
    spans = lax.broadcasted_iota(jnp.int32, (users, 128), 0)
    limits = jnp.zeros((users, 128), jnp.int32)
    for u in range(users):
        limits = jnp.where(spans == u, lengths[u], limits)
    lane = lax.broadcasted_iota(jnp.int32, (users, 128), 1)
    found = jnp.zeros((users, 128), jnp.int32)
    chosen = picks[...]
    for b in range(blocks):
        hit = jnp.max(jnp.where(chosen == me * blocks + b, 1.0, 0.0), axis=1, keepdims=True)
        found = jnp.where(jnp.logical_and(lane == b, hit > 0.0), 1, found)
    flags[...] = jnp.where((me * blocks + lane) * BLOCK < limits, found, 0)
    locals_[0].wait()
    for copy in weight_copies:
        copy.wait()
    key_weight, value_weight = all_proj[1], all_proj[2]
    shape = (blocks, BLOCK, embed)
    places = lax.broadcasted_iota(jnp.int32, shape, 0) * BLOCK + lax.broadcasted_iota(jnp.int32, shape, 1)
    places = places + me * own_rows
    for u in range(users):
        for k in range(line - 1):
            along[k, u].wait_recv()
            source = lax.rem(spot + line - (k + 1), line) * 2 + side
            copy = pltpu.make_async_remote_copy(
                place(u, source),
                place(u, source),
                y_send.at[k + 1, u],
                y_recv.at[k + 1, u],
                device_id={"hist": partner},
                device_id_type=mesh_id,
            )
            copy.start()
            across[k + 1, u] = copy
        fetches[u].wait()
        block_rows = rows_in[u].reshape(shape).astype(jnp.float32)
        alive = places < lengths[u]
        safe = jnp.where(alive, block_rows, block_rows[:, 0:1, :]).astype(jnp.bfloat16).reshape(own_rows, embed)
        kept = jnp.where(alive, block_rows, 0.0).astype(jnp.bfloat16).reshape(own_rows, embed)
        keys[u] = jnp.dot(safe, key_weight, preferred_element_type=jnp.float32).astype(jnp.bfloat16)
        values[u] = lax.dot_general(
            value_weight, kept, (((0,), (1,)), ((), ())), preferred_element_type=jnp.float32
        ).astype(jnp.bfloat16)
    for u in range(users):
        for k in range(line):
            across[k, u].wait_recv()
        locals_[1 + u].wait()
        plain = lax.dot_general(
            all_proj[0], all_cand[u], (((0,), (1,)), ((), ())), preferred_element_type=jnp.float32
        ).astype(jnp.bfloat16)
        scaled = plain.astype(jnp.float32) * factor
        upper = scaled.astype(jnp.bfloat16)
        high[u] = upper
        low[u] = (scaled - upper.astype(jnp.float32)).astype(jnp.bfloat16)
    for copy in list(along.values()) + list(across.values()):
        copy.wait_send()


def attend_kernel(
    own_cands,
    lengths,
    flags,
    base,
    high,
    low,
    keys,
    values,
    parts,
    stats,
    marks,
    acc,
    shift,
    top,
    probs,
    slots,
    owners,
):
    users, embed, cands = high.shape
    head = embed // H
    half = embed // 2
    tall = acc[0].shape[1]
    blocks = keys.shape[1] // BLOCK
    first = base[0]

    owners[0] = 0
    slots[0] = PAD
    slots[1] = PAD
    item = jnp.int32(1)
    begins, counts = [], []
    for u in range(users):
        last = jnp.int32(0)
        at = item * PAIR
        begins.append(item)
        for b in range(blocks):
            alive = flags[u, b]
            slots[at] = b
            at = at + alive
            last = jnp.where(alive > 0, b, last)
        for k in range(3 * PAIR):
            slots[at + k] = last + PAD
        for p in range(blocks // PAIR + 3):
            owners[item + p] = u
        counts.append(at - item * PAIR)
        item = (at + 1) // PAIR
    trips = (item - 1 + TRIP - 1) // TRIP

    def start_of(slot):
        block = jnp.where(slot >= PAD, slot - PAD, slot)
        return pl.multiple_of(block * BLOCK, BLOCK)

    column = lax.broadcasted_iota(jnp.int32, (1, embed), 1)
    group = [(h * head) // half for h in range(H)]
    spot = [(1 - group[h]) * half + (h - group[h] * (H // 2)) * 16 for h in range(H)]
    mine = [jnp.where(column // head == h, 1.0, 0.0).astype(jnp.bfloat16) for h in range(H)]
    mark = [jnp.where(column == spot[h], 1.0, 0.0).astype(jnp.bfloat16) for h in range(H)]
    lead = lax.broadcasted_iota(jnp.int32, (16, cands), 0) == 0

    for u in range(users):
        sample = keys[u, pl.ds(start_of(slots[begins[u] * PAIR]), SAMPLE), :]
        guess = jnp.dot(
            jnp.concatenate([sample * mine[h] for h in range(H)], axis=0), high[u], preferred_element_type=jnp.float32
        )
        for h in range(H):
            most = jnp.max(guess[h * SAMPLE : (h + 1) * SAMPLE, :], axis=0, keepdims=True)
            most = most.astype(jnp.bfloat16).astype(jnp.float32)
            shift[h][u] = most
            marks[h][u] = jnp.where(lead, -most, 0.0).astype(jnp.bfloat16)
    for h in range(H):
        acc[h][...] = jnp.zeros(acc[h].shape, jnp.float32)
    for k in range(2):
        probs[2 + k][...] = jnp.zeros(probs[2 + k].shape, jnp.bfloat16)

    right = lax.broadcasted_iota(jnp.int32, (tall - head, BLOCK), 1)
    under = lax.broadcasted_iota(jnp.int32, (tall - head, BLOCK), 0)
    right = jnp.where(under == 0, right, jnp.iinfo(jnp.int32).max)

    def scores(i, h):
        user = owners[i]
        key = jnp.concatenate([keys[user, pl.ds(start_of(slots[i * PAIR + k]), BLOCK), :] for k in range(PAIR)], axis=0)
        key = key * mine[h]
        pieces = [high[user]]
        if spot[h] > 0:
            pieces.append(low[user, 0 : spot[h], :])
        pieces += [marks[h][user], low[user, spot[h] + 16 : embed, :]]
        query = jnp.concatenate(pieces, axis=0)
        return jnp.dot(jnp.concatenate([key, key + mark[h]], axis=1), query, preferred_element_type=jnp.float32)

    def gain(i, h, prob):
        user = owners[i]
        pieces = []
        for k in range(PAIR):
            slot = slots[i * PAIR + k]
            start = start_of(slot)
            limit = jnp.where(slot >= PAD, 0, lengths[user] - (start + first * BLOCK))
            one = jnp.where(right < limit, 1.0, 0.0).astype(jnp.bfloat16)
            value = values[user, h * head : (h + 1) * head, pl.ds(start, BLOCK)]
            value = jnp.where(slot >= PAD, jnp.zeros_like(value), value)
            pieces.append(jnp.concatenate([value, one], axis=0))
        return jnp.dot(jnp.concatenate(pieces, axis=1), prob, preferred_element_type=jnp.float32)

    @pl.loop(0, trips)
    def _(step):
        begin = step * TRIP + 1
        for s in range(TRIP * H):
            late, head_late = begin + (s + 2 * H - LAG) // H - 2, (s + H - LAG) % H
            probs[s % 4][...] = jnp.exp2(scores(begin + s // H, s % H)).astype(jnp.bfloat16)
            acc[head_late][owners[late]] += gain(late, head_late, probs[(s - LAG) % 4][...])

    for k in range(LAG):
        h = H - LAG + k
        user = owners[trips * TRIP]
        acc[h][user] += gain(trips * TRIP, h, probs[(TRIP * H - LAG + k) % 4][...])

    wrong = jnp.zeros((1, cands), jnp.float32)
    for u in range(users):
        for h in range(H):
            amount = acc[h][u, head : head + 1, :]
            fine = jnp.logical_and(amount > SMALL, amount < LARGE)
            wrong = jnp.maximum(wrong, jnp.where(fine, 0.0, jnp.where(counts[u] > 0, 1.0, 0.0)))

    @pl.when(jnp.max(wrong) > 0.0)
    def _():
        for h in range(H):
            acc[h][...] = jnp.zeros(acc[h].shape, jnp.float32)
            top[h][...] = jnp.full(top[h].shape, LOW, jnp.float32)

        @pl.loop(1, item)
        def _(i):
            user = owners[i]
            for h in range(H):
                got = scores(i, h)
                before = top[h][user]
                peak = jnp.maximum(before, jnp.max(got, axis=0, keepdims=True))
                prob = jnp.exp2(got - peak).astype(jnp.bfloat16)
                acc[h][user] = acc[h][user] * jnp.exp2(before - peak) + gain(i, h, prob)
                top[h][user] = peak

        for h in range(H):
            shift[h][...] = shift[h][...] + top[h][...]

    means, logs = [], []
    for u in range(users):
        rows, row_logs = [], []
        for h in range(H):
            amount = acc[h][u, head : head + 1, :]
            some = jnp.logical_and(counts[u] > 0, amount > 0.0)
            safe = jnp.where(some, amount, 1.0)
            mean = jnp.where(some, acc[h][u, 0:head, :] * (1.0 / safe), 0.0)
            rows.append(mean.astype(jnp.bfloat16))
            row_logs.append(jnp.where(some, shift[h][u] + jnp.log2(safe), LOW))
        means.append(jnp.concatenate(rows, axis=0))
        logs.append(jnp.concatenate(row_logs, axis=0))
    for dest in range(parts.shape[0]):
        at = slice(dest * own_cands, (dest + 1) * own_cands)
        to = slice(0, users * own_cands)
        parts[dest, :, to] = jnp.concatenate([m[:, at] for m in means], axis=1)
        stats[dest, :, to] = jnp.concatenate([m[:, at] for m in logs], axis=1)


def combine_kernel(n, parts, stats, out_weight, result, got, got_stats, send_a, recv_a, send_b, recv_b):
    me = lax.axis_index("hist")
    barrier = pltpu.get_barrier_semaphore()
    for k in range(1, n):
        pl.semaphore_signal(
            barrier, inc=1, device_id={"hist": lax.rem(me + k, n)}, device_id_type=pl.DeviceIdType.MESH
        )
    pl.semaphore_wait(barrier, n - 1)
    copies = []
    for k in range(1, n):
        peer = lax.rem(me + k, n)
        for src, dst, send, recv in ((stats, got_stats, send_b, recv_b), (parts, got, send_a, recv_a)):
            copy = pltpu.make_async_remote_copy(
                src_ref=src.at[peer],
                dst_ref=dst.at[k - 1],
                send_sem=send.at[k - 1],
                recv_sem=recv.at[k - 1],
                device_id={"hist": peer},
                device_id_type=pl.DeviceIdType.MESH,
            )
            copy.start()
            copies.append(copy)
    for copy in copies:
        copy.wait()
    logs = [stats[me]] + [got_stats[k] for k in range(n - 1)]
    highest = functools.reduce(jnp.maximum, logs)
    shares = [jnp.exp2(log - highest) for log in logs]
    inverse = 1.0 / functools.reduce(jnp.add, shares)
    embed = parts.shape[1]
    head = embed // H
    pieces = []
    for h in range(H):
        rows = slice(h * head, (h + 1) * head)
        mixed = parts[me, rows, :].astype(jnp.float32) * shares[0][h : h + 1, :]
        for k in range(n - 1):
            mixed += got[k, rows, :].astype(jnp.float32) * shares[k + 1][h : h + 1, :]
        pieces.append(mixed * inverse[h : h + 1, :])
    attended = jnp.concatenate(pieces, axis=0).astype(jnp.bfloat16)
    result[...] = lax.dot_general(
        attended, out_weight[3], (((0,), (0,)), ((), ())), preferred_element_type=jnp.float32
    ).astype(jnp.bfloat16)


def body(candidates, history, projections, lengths, selected):
    n = lax.axis_size("hist")
    ranks = lax.axis_size("dp")
    candidates, history, projections, lengths, selected = (
        pltpu.with_memory_space_constraint(x, pltpu.HBM) for x in (candidates, history, projections, lengths, selected)
    )
    users, own_cands, embed = candidates.shape
    cands = n * own_cands
    line = n // 2
    own_rows = history.shape[1]
    blocks = own_rows // BLOCK
    first = (lax.axis_index("hist") * blocks).astype(jnp.int32)
    base = first.reshape(1)
    weights, high, low, keys, values, flags = pl.pallas_call(
        functools.partial(gather_kernel, n, ranks),
        out_shape=[
            pltpu.VMEM((projections.shape[0], ranks * projections.shape[1], embed), jnp.bfloat16),
            pltpu.VMEM((users, embed, cands), jnp.bfloat16),
            pltpu.VMEM((users, embed, cands), jnp.bfloat16),
            pltpu.VMEM((users, own_rows, embed), jnp.bfloat16),
            pltpu.VMEM((users, embed, own_rows), jnp.bfloat16),
            jax.ShapeDtypeStruct((users, 128), jnp.int32),
        ],
        in_specs=[pl.BlockSpec(memory_space=pltpu.SMEM)] + [pl.BlockSpec(memory_space=pltpu.HBM)] * 4,
        out_specs=[pl.BlockSpec(memory_space=pltpu.VMEM)] * 6,
        scratch_shapes=[
            pltpu.VMEM(candidates.shape, jnp.bfloat16),
            pltpu.VMEM(projections.shape, jnp.bfloat16),
            pltpu.VMEM(selected.shape, jnp.int32),
            pltpu.VMEM((users, cands, embed), jnp.bfloat16),
            pltpu.VMEM((users, own_rows, embed), jnp.bfloat16),
            pltpu.SemaphoreType.DMA((users + 1,)),
            pltpu.SemaphoreType.DMA((3,)),
            pltpu.SemaphoreType.DMA((users,)),
            pltpu.SemaphoreType.DMA((line - 1, users)),
            pltpu.SemaphoreType.DMA((line - 1, users)),
            pltpu.SemaphoreType.DMA((line, users)),
            pltpu.SemaphoreType.DMA((line, users)),
            pltpu.SemaphoreType.DMA((ranks - 1,)),
            pltpu.SemaphoreType.DMA((ranks - 1,)),
        ],
        compiler_params=pltpu.CompilerParams(collective_id=1, has_side_effects=True, vmem_limit_bytes=ROOM),
        name="gather",
    )(lengths, candidates, projections, history, selected)
    wide = -(-users * own_cands // 128) * 128
    parts, stats = pl.pallas_call(
        functools.partial(attend_kernel, own_cands),
        in_specs=[pl.BlockSpec(memory_space=pltpu.SMEM)] * 3 + [pl.BlockSpec(memory_space=pltpu.VMEM)] * 4,
        out_specs=[pl.BlockSpec(memory_space=pltpu.VMEM)] * 2,
        scratch_shapes=[
            [pltpu.VMEM((users, 16, cands), jnp.bfloat16)] * H,
            [pltpu.VMEM((users, embed // H + 16, cands), jnp.float32)] * H,
            [pltpu.VMEM((users, 1, cands), jnp.float32)] * H,
            [pltpu.VMEM((users, 1, cands), jnp.float32)] * H,
            [pltpu.VMEM((PAIR * BLOCK, cands), jnp.bfloat16)] * 4,
            pltpu.SMEM(((users * blocks) + users * PAIR + 8 * PAIR,), jnp.int32),
            pltpu.SMEM((users * (blocks // PAIR + 1) + 8,), jnp.int32),
        ],
        out_shape=[
            pltpu.VMEM((n, embed, wide), jnp.bfloat16),
            pltpu.VMEM((n, H, wide), jnp.float32),
        ],
        compiler_params=pltpu.CompilerParams(vmem_limit_bytes=ROOM),
        name="attend",
    )(lengths, flags, base, high, low, keys, values)
    result = pl.pallas_call(
        functools.partial(combine_kernel, n),
        out_shape=jax.ShapeDtypeStruct((wide, embed), jnp.bfloat16),
        in_specs=[pl.BlockSpec(memory_space=pltpu.VMEM)] * 3,
        out_specs=pl.BlockSpec(memory_space=pltpu.VMEM),
        scratch_shapes=[
            pltpu.VMEM((n - 1, embed, wide), jnp.bfloat16),
            pltpu.VMEM((n - 1, H, wide), jnp.float32),
        ]
        + [pltpu.SemaphoreType.DMA((n - 1,))] * 4,
        compiler_params=pltpu.CompilerParams(collective_id=0, has_side_effects=True, vmem_limit_bytes=ROOM),
        name="combine",
    )(parts, stats, weights)
    return result[: users * own_cands].reshape(users, own_cands, embed)


def solution(mesh):
    placed = (
        P("dp", "hist", None),
        P("dp", "hist", None),
        P(None, "dp", None),
        P("dp"),
        P("dp", None),
    )
    return jax.shard_map(
        body, mesh=mesh, in_specs=placed, out_specs=P("dp", "hist", None), check_vma=False
    )
```

```python
import functools
import math

import jax
import jax.numpy as jnp
from jax import lax
from jax.experimental import pallas as pl
from jax.experimental.pallas import tpu as pltpu
from jax.sharding import PartitionSpec as P

H = 4
BLOCK = 128
PAIR = 2
TRIP = 2
PAD = 1 << 20
LAG = 2
SAMPLE = 32
SMALL = 2.0**-30
LARGE = 2.0**100
ROOM = 40 << 20
LOW = -1e30


def gather_kernel(
    n,
    ranks,
    lengths,
    cand_in,
    proj_in,
    hist,
    picks_in,
    all_proj,
    query,
    keys,
    values,
    flags,
    cand,
    proj,
    picks,
    all_cand,
    rows_in,
    own_sem,
    arg_sem,
    in_sem,
    z_send,
    z_recv,
    y_send,
    y_recv,
    w_send,
    w_recv,
):
    mesh_id = pl.DeviceIdType.MESH
    me, rank = lax.axis_index("hist"), lax.axis_index("dp")
    line = n // 2
    side, spot = lax.rem(me, 2), me // 2
    users, own = cand.shape[0], cand.shape[1]
    rows = proj.shape[1]
    own_rows, embed = hist.shape[1], hist.shape[2]
    blocks = own_rows // BLOCK

    def place(u, owner):
        return all_cand.at[u, pl.ds(pl.multiple_of(owner * own, own), own), :]

    loads = [
        pltpu.make_async_copy(src, dst, arg_sem.at[k])
        for k, (src, dst) in enumerate(((proj_in, proj), (cand_in, cand), (picks_in, picks)))
    ]
    strip = all_proj.at[:, pl.ds(pl.multiple_of(rank * rows, rows), rows), :]
    locals_ = [pltpu.make_async_copy(proj_in, strip, own_sem.at[users])]
    locals_ += [pltpu.make_async_copy(cand_in.at[u], place(u, me), own_sem.at[u]) for u in range(users)]
    fetches = [pltpu.make_async_copy(hist.at[u], rows_in.at[u], in_sem.at[u]) for u in range(users)]
    for copy in loads + locals_ + fetches:
        copy.start()
    partner = spot * 2 + (1 - side)
    peers = [lax.rem(spot + k, line) * 2 + side for k in range(1, line)]
    mates = [lax.rem(rank + k, ranks) for k in range(1, ranks)]

    barrier = pltpu.get_barrier_semaphore()
    for peer in [partner] + peers:
        pl.semaphore_signal(barrier, inc=1, device_id={"hist": peer}, device_id_type=mesh_id)
    for mate in mates:
        pl.semaphore_signal(barrier, inc=1, device_id={"dp": mate}, device_id_type=mesh_id)
    pl.semaphore_wait(barrier, line + ranks - 1)

    loads[0].wait()
    loads[1].wait()
    weight_copies = []
    for k, mate in enumerate(mates):
        copy = pltpu.make_async_remote_copy(
            proj, strip, w_send.at[k], w_recv.at[k], device_id={"dp": mate}, device_id_type=mesh_id
        )
        copy.start()
        weight_copies.append(copy)
    across, along = {}, {}
    for u in range(users):
        for k, peer in enumerate(peers):
            copy = pltpu.make_async_remote_copy(
                cand.at[u],
                place(u, me),
                z_send.at[k, u],
                z_recv.at[k, u],
                device_id={"hist": peer},
                device_id_type=mesh_id,
            )
            copy.start()
            along[k, u] = copy
        copy = pltpu.make_async_remote_copy(
            cand.at[u],
            place(u, me),
            y_send.at[0, u],
            y_recv.at[0, u],
            device_id={"hist": partner},
            device_id_type=mesh_id,
        )
        copy.start()
        across[0, u] = copy
    loads[2].wait()
    spans = lax.broadcasted_iota(jnp.int32, (users, 128), 0)
    limits = jnp.zeros((users, 128), jnp.int32)
    for u in range(users):
        limits = jnp.where(spans == u, lengths[u], limits)
    lane = lax.broadcasted_iota(jnp.int32, (users, 128), 1)
    found = jnp.zeros((users, 128), jnp.int32)
    chosen = picks[...]
    for b in range(blocks):
        hit = jnp.max(jnp.where(chosen == me * blocks + b, 1.0, 0.0), axis=1, keepdims=True)
        found = jnp.where(jnp.logical_and(lane == b, hit > 0.0), 1, found)
    flags[...] = jnp.where((me * blocks + lane) * BLOCK < limits, found, 0)
    locals_[0].wait()
    for copy in weight_copies:
        copy.wait()
    key_weight, value_weight = all_proj[1], all_proj[2]
    shape = (blocks, BLOCK, embed)
    places = lax.broadcasted_iota(jnp.int32, shape, 0) * BLOCK + lax.broadcasted_iota(jnp.int32, shape, 1)
    places = places + me * own_rows
    for u in range(users):
        for k in range(line - 1):
            along[k, u].wait_recv()
            source = lax.rem(spot + line - (k + 1), line) * 2 + side
            copy = pltpu.make_async_remote_copy(
                place(u, source),
                place(u, source),
                y_send.at[k + 1, u],
                y_recv.at[k + 1, u],
                device_id={"hist": partner},
                device_id_type=mesh_id,
            )
            copy.start()
            across[k + 1, u] = copy
        fetches[u].wait()
        block_rows = rows_in[u].reshape(shape).astype(jnp.float32)
        alive = places < lengths[u]
        safe = jnp.where(alive, block_rows, block_rows[:, 0:1, :]).astype(jnp.bfloat16).reshape(own_rows, embed)
        kept = jnp.where(alive, block_rows, 0.0).astype(jnp.bfloat16).reshape(own_rows, embed)
        keys[u] = jnp.dot(safe, key_weight, preferred_element_type=jnp.float32).astype(jnp.bfloat16)
        values[u] = lax.dot_general(
            value_weight, kept, (((0,), (1,)), ((), ())), preferred_element_type=jnp.float32
        ).astype(jnp.bfloat16)
    for u in range(users):
        for k in range(line):
            across[k, u].wait_recv()
        locals_[1 + u].wait()
        query[u] = lax.dot_general(
            all_proj[0], all_cand[u], (((0,), (1,)), ((), ())), preferred_element_type=jnp.float32
        ).astype(jnp.bfloat16)
    for copy in list(along.values()) + list(across.values()):
        copy.wait_send()


def attend_kernel(
    own_cands,
    lengths,
    flags,
    base,
    query,
    keys,
    values,
    parts,
    stats,
    acc,
    shift,
    top,
    probs,
    slots,
    owners,
):
    users, embed, cands = query.shape
    head = embed // H
    tall = acc[0].shape[1]
    blocks = keys.shape[1] // BLOCK
    factor = math.log2(math.e) / math.sqrt(head)
    first = base[0]

    owners[0] = 0
    slots[0] = PAD
    slots[1] = PAD
    item = jnp.int32(1)
    begins, counts = [], []
    for u in range(users):
        last = jnp.int32(0)
        at = item * PAIR
        begins.append(item)
        for b in range(blocks):
            alive = flags[u, b]
            slots[at] = b
            at = at + alive
            last = jnp.where(alive > 0, b, last)
        for k in range(3 * PAIR):
            slots[at + k] = last + PAD
        for p in range(blocks // PAIR + 3):
            owners[item + p] = u
        counts.append(at - item * PAIR)
        item = (at + 1) // PAIR
    trips = (item - 1 + TRIP - 1) // TRIP

    def start_of(slot):
        block = jnp.where(slot >= PAD, slot - PAD, slot)
        return pl.multiple_of(block * BLOCK, BLOCK)

    column = lax.broadcasted_iota(jnp.int32, (1, embed), 1)
    mine = [jnp.where(column // head == h, 1.0, 0.0).astype(jnp.bfloat16) for h in range(H)]

    for u in range(users):
        sample = keys[u, pl.ds(start_of(slots[begins[u] * PAIR]), SAMPLE), :]
        guess = jnp.dot(
            jnp.concatenate([sample * mine[h] for h in range(H)], axis=0), query[u], preferred_element_type=jnp.float32
        )
        for h in range(H):
            most = jnp.max(guess[h * SAMPLE : (h + 1) * SAMPLE, :], axis=0, keepdims=True)
            shift[h][u] = most * factor
    for h in range(H):
        acc[h][...] = jnp.zeros(acc[h].shape, jnp.float32)
    for k in range(2):
        probs[2 + k][...] = jnp.zeros(probs[2 + k].shape, jnp.bfloat16)

    right = lax.broadcasted_iota(jnp.int32, (tall - head, BLOCK), 1)
    under = lax.broadcasted_iota(jnp.int32, (tall - head, BLOCK), 0)
    right = jnp.where(under == 0, right, jnp.iinfo(jnp.int32).max)

    def scores(i, h):
        user = owners[i]
        key = jnp.concatenate([keys[user, pl.ds(start_of(slots[i * PAIR + k]), BLOCK), :] for k in range(PAIR)], axis=0)
        got = jnp.dot(key * mine[h], query[user], preferred_element_type=jnp.float32)
        return got * factor - shift[h][user]

    def gain(i, h, prob):
        user = owners[i]
        pieces = []
        for k in range(PAIR):
            slot = slots[i * PAIR + k]
            start = start_of(slot)
            limit = jnp.where(slot >= PAD, 0, lengths[user] - (start + first * BLOCK))
            one = jnp.where(right < limit, 1.0, 0.0).astype(jnp.bfloat16)
            value = values[user, h * head : (h + 1) * head, pl.ds(start, BLOCK)]
            value = jnp.where(slot >= PAD, jnp.zeros_like(value), value)
            pieces.append(jnp.concatenate([value, one], axis=0))
        return jnp.dot(jnp.concatenate(pieces, axis=1), prob, preferred_element_type=jnp.float32)

    @pl.loop(0, trips)
    def _(step):
        begin = step * TRIP + 1
        for s in range(TRIP * H):
            late, head_late = begin + (s + 2 * H - LAG) // H - 2, (s + H - LAG) % H
            probs[s % 4][...] = jnp.exp2(scores(begin + s // H, s % H)).astype(jnp.bfloat16)
            acc[head_late][owners[late]] += gain(late, head_late, probs[(s - LAG) % 4][...])

    for k in range(LAG):
        h = H - LAG + k
        user = owners[trips * TRIP]
        acc[h][user] += gain(trips * TRIP, h, probs[(TRIP * H - LAG + k) % 4][...])

    wrong = jnp.zeros((1, cands), jnp.float32)
    for u in range(users):
        for h in range(H):
            amount = acc[h][u, head : head + 1, :]
            fine = jnp.logical_and(amount > SMALL, amount < LARGE)
            wrong = jnp.maximum(wrong, jnp.where(fine, 0.0, jnp.where(counts[u] > 0, 1.0, 0.0)))

    @pl.when(jnp.max(wrong) > 0.0)
    def _():
        for h in range(H):
            acc[h][...] = jnp.zeros(acc[h].shape, jnp.float32)
            top[h][...] = jnp.full(top[h].shape, LOW, jnp.float32)

        @pl.loop(1, item)
        def _(i):
            user = owners[i]
            for h in range(H):
                got = scores(i, h)
                before = top[h][user]
                peak = jnp.maximum(before, jnp.max(got, axis=0, keepdims=True))
                prob = jnp.exp2(got - peak).astype(jnp.bfloat16)
                acc[h][user] = acc[h][user] * jnp.exp2(before - peak) + gain(i, h, prob)
                top[h][user] = peak

        for h in range(H):
            shift[h][...] = shift[h][...] + top[h][...]

    means, logs = [], []
    for u in range(users):
        rows, row_logs = [], []
        for h in range(H):
            amount = acc[h][u, head : head + 1, :]
            some = jnp.logical_and(counts[u] > 0, amount > 0.0)
            safe = jnp.where(some, amount, 1.0)
            mean = jnp.where(some, acc[h][u, 0:head, :] * (1.0 / safe), 0.0)
            rows.append(mean.astype(jnp.bfloat16))
            row_logs.append(jnp.where(some, shift[h][u] + jnp.log2(safe), LOW))
        means.append(jnp.concatenate(rows, axis=0))
        logs.append(jnp.concatenate(row_logs, axis=0))
    for dest in range(parts.shape[0]):
        at = slice(dest * own_cands, (dest + 1) * own_cands)
        to = slice(0, users * own_cands)
        parts[dest, :, to] = jnp.concatenate([m[:, at] for m in means], axis=1)
        stats[dest, :, to] = jnp.concatenate([m[:, at] for m in logs], axis=1)


def combine_kernel(n, parts, stats, out_weight, result, got, got_stats, send_a, recv_a, send_b, recv_b):
    me = lax.axis_index("hist")
    barrier = pltpu.get_barrier_semaphore()
    for k in range(1, n):
        pl.semaphore_signal(
            barrier, inc=1, device_id={"hist": lax.rem(me + k, n)}, device_id_type=pl.DeviceIdType.MESH
        )
    pl.semaphore_wait(barrier, n - 1)
    copies = []
    for k in range(1, n):
        peer = lax.rem(me + k, n)
        for src, dst, send, recv in ((stats, got_stats, send_b, recv_b), (parts, got, send_a, recv_a)):
            copy = pltpu.make_async_remote_copy(
                src_ref=src.at[peer],
                dst_ref=dst.at[k - 1],
                send_sem=send.at[k - 1],
                recv_sem=recv.at[k - 1],
                device_id={"hist": peer},
                device_id_type=pl.DeviceIdType.MESH,
            )
            copy.start()
            copies.append(copy)
    for copy in copies:
        copy.wait()
    logs = [stats[me]] + [got_stats[k] for k in range(n - 1)]
    highest = functools.reduce(jnp.maximum, logs)
    shares = [jnp.exp2(log - highest) for log in logs]
    inverse = 1.0 / functools.reduce(jnp.add, shares)
    embed = parts.shape[1]
    head = embed // H
    pieces = []
    for h in range(H):
        rows = slice(h * head, (h + 1) * head)
        mixed = parts[me, rows, :].astype(jnp.float32) * shares[0][h : h + 1, :]
        for k in range(n - 1):
            mixed += got[k, rows, :].astype(jnp.float32) * shares[k + 1][h : h + 1, :]
        pieces.append(mixed * inverse[h : h + 1, :])
    attended = jnp.concatenate(pieces, axis=0).astype(jnp.bfloat16)
    result[...] = lax.dot_general(
        attended, out_weight[3], (((0,), (0,)), ((), ())), preferred_element_type=jnp.float32
    ).astype(jnp.bfloat16)


def body(candidates, history, projections, lengths, selected):
    n = lax.axis_size("hist")
    ranks = lax.axis_size("dp")
    candidates, history, projections, lengths, selected = (
        pltpu.with_memory_space_constraint(x, pltpu.HBM) for x in (candidates, history, projections, lengths, selected)
    )
    users, own_cands, embed = candidates.shape
    cands = n * own_cands
    line = n // 2
    own_rows = history.shape[1]
    blocks = own_rows // BLOCK
    first = (lax.axis_index("hist") * blocks).astype(jnp.int32)
    base = first.reshape(1)
    weights, query, keys, values, flags = pl.pallas_call(
        functools.partial(gather_kernel, n, ranks),
        out_shape=[
            pltpu.VMEM((projections.shape[0], ranks * projections.shape[1], embed), jnp.bfloat16),
            pltpu.VMEM((users, embed, cands), jnp.bfloat16),
            pltpu.VMEM((users, own_rows, embed), jnp.bfloat16),
            pltpu.VMEM((users, embed, own_rows), jnp.bfloat16),
            jax.ShapeDtypeStruct((users, 128), jnp.int32),
        ],
        in_specs=[pl.BlockSpec(memory_space=pltpu.SMEM)] + [pl.BlockSpec(memory_space=pltpu.HBM)] * 4,
        out_specs=[pl.BlockSpec(memory_space=pltpu.VMEM)] * 5,
        scratch_shapes=[
            pltpu.VMEM(candidates.shape, jnp.bfloat16),
            pltpu.VMEM(projections.shape, jnp.bfloat16),
            pltpu.VMEM(selected.shape, jnp.int32),
            pltpu.VMEM((users, cands, embed), jnp.bfloat16),
            pltpu.VMEM((users, own_rows, embed), jnp.bfloat16),
            pltpu.SemaphoreType.DMA((users + 1,)),
            pltpu.SemaphoreType.DMA((3,)),
            pltpu.SemaphoreType.DMA((users,)),
            pltpu.SemaphoreType.DMA((line - 1, users)),
            pltpu.SemaphoreType.DMA((line - 1, users)),
            pltpu.SemaphoreType.DMA((line, users)),
            pltpu.SemaphoreType.DMA((line, users)),
            pltpu.SemaphoreType.DMA((ranks - 1,)),
            pltpu.SemaphoreType.DMA((ranks - 1,)),
        ],
        compiler_params=pltpu.CompilerParams(collective_id=1, has_side_effects=True, vmem_limit_bytes=ROOM),
        name="gather",
    )(lengths, candidates, projections, history, selected)
    wide = -(-users * own_cands // 128) * 128
    parts, stats = pl.pallas_call(
        functools.partial(attend_kernel, own_cands),
        in_specs=[pl.BlockSpec(memory_space=pltpu.SMEM)] * 3 + [pl.BlockSpec(memory_space=pltpu.VMEM)] * 3,
        out_specs=[pl.BlockSpec(memory_space=pltpu.VMEM)] * 2,
        scratch_shapes=[
            [pltpu.VMEM((users, embed // H + 16, cands), jnp.float32)] * H,
            [pltpu.VMEM((users, 1, cands), jnp.float32)] * H,
            [pltpu.VMEM((users, 1, cands), jnp.float32)] * H,
            [pltpu.VMEM((PAIR * BLOCK, cands), jnp.bfloat16)] * 4,
            pltpu.SMEM(((users * blocks) + users * PAIR + 8 * PAIR,), jnp.int32),
            pltpu.SMEM((users * (blocks // PAIR + 1) + 8,), jnp.int32),
        ],
        out_shape=[
            pltpu.VMEM((n, embed, wide), jnp.bfloat16),
            pltpu.VMEM((n, H, wide), jnp.float32),
        ],
        compiler_params=pltpu.CompilerParams(vmem_limit_bytes=ROOM),
        name="attend",
    )(lengths, flags, base, query, keys, values)
    result = pl.pallas_call(
        functools.partial(combine_kernel, n),
        out_shape=jax.ShapeDtypeStruct((wide, embed), jnp.bfloat16),
        in_specs=[pl.BlockSpec(memory_space=pltpu.VMEM)] * 3,
        out_specs=pl.BlockSpec(memory_space=pltpu.VMEM),
        scratch_shapes=[
            pltpu.VMEM((n - 1, embed, wide), jnp.bfloat16),
            pltpu.VMEM((n - 1, H, wide), jnp.float32),
        ]
        + [pltpu.SemaphoreType.DMA((n - 1,))] * 4,
        compiler_params=pltpu.CompilerParams(collective_id=0, has_side_effects=True, vmem_limit_bytes=ROOM),
        name="combine",
    )(parts, stats, weights)
    return result[: users * own_cands].reshape(users, own_cands, embed)


def solution(mesh):
    placed = (
        P("dp", "hist", None),
        P("dp", "hist", None),
        P(None, "dp", None),
        P("dp"),
        P("dp", None),
    )
    return jax.shard_map(
        body, mesh=mesh, in_specs=placed, out_specs=P("dp", "hist", None), check_vma=False
    )
```

```python
import functools
import math

import jax
import jax.numpy as jnp
from jax import lax
from jax.experimental import pallas as pl
from jax.experimental.pallas import tpu as pltpu
from jax.sharding import PartitionSpec as P

H = 4
BLOCK = 128
PAIR = 2
TRIP = 2
PAD = 1 << 20
LAG = 2
SAMPLE = 32
SMALL = 2.0**-30
LARGE = 2.0**100
ROOM = 40 << 20
LANES = 128
LOW = -1e30


def gather_kernel(
    n,
    ranks,
    lengths,
    cand_in,
    proj_in,
    hist,
    picks_in,
    all_proj,
    query,
    keys,
    values,
    flags,
    cand,
    proj,
    picks,
    all_cand,
    rows_in,
    own_sem,
    arg_sem,
    in_sem,
    z_send,
    z_recv,
    y_send,
    y_recv,
    w_send,
    w_recv,
):
    mesh_id = pl.DeviceIdType.MESH
    me, rank = lax.axis_index("hist"), lax.axis_index("dp")
    line = n // 2
    side, spot = lax.rem(me, 2), me // 2
    users, own = cand.shape[0], cand.shape[1]
    rows = proj.shape[1]
    own_rows, embed = hist.shape[1], hist.shape[2]
    blocks = own_rows // BLOCK

    def place(u, owner):
        return all_cand.at[u, pl.ds(pl.multiple_of(owner * own, own), own), :]

    loads = [
        pltpu.make_async_copy(src, dst, arg_sem.at[k])
        for k, (src, dst) in enumerate(((proj_in, proj), (cand_in, cand), (picks_in, picks)))
    ]
    strip = all_proj.at[:, pl.ds(pl.multiple_of(rank * rows, rows), rows), :]
    locals_ = [pltpu.make_async_copy(proj_in, strip, own_sem.at[users])]
    locals_ += [pltpu.make_async_copy(cand_in.at[u], place(u, me), own_sem.at[u]) for u in range(users)]
    fetches = [pltpu.make_async_copy(hist.at[u], rows_in.at[u], in_sem.at[u]) for u in range(users)]
    for copy in loads + locals_ + fetches:
        copy.start()
    partner = spot * 2 + (1 - side)
    peers = [lax.rem(spot + k, line) * 2 + side for k in range(1, line)]
    mates = [lax.rem(rank + k, ranks) for k in range(1, ranks)]

    barrier = pltpu.get_barrier_semaphore()
    for peer in [partner] + peers:
        pl.semaphore_signal(barrier, inc=1, device_id={"hist": peer}, device_id_type=mesh_id)
    for mate in mates:
        pl.semaphore_signal(barrier, inc=1, device_id={"dp": mate}, device_id_type=mesh_id)
    pl.semaphore_wait(barrier, line + ranks - 1)

    loads[0].wait()
    loads[1].wait()
    weight_copies = []
    for k, mate in enumerate(mates):
        copy = pltpu.make_async_remote_copy(
            proj, strip, w_send.at[k], w_recv.at[k], device_id={"dp": mate}, device_id_type=mesh_id
        )
        copy.start()
        weight_copies.append(copy)
    across, along = {}, {}
    for u in range(users):
        for k, peer in enumerate(peers):
            copy = pltpu.make_async_remote_copy(
                cand.at[u],
                place(u, me),
                z_send.at[k, u],
                z_recv.at[k, u],
                device_id={"hist": peer},
                device_id_type=mesh_id,
            )
            copy.start()
            along[k, u] = copy
        copy = pltpu.make_async_remote_copy(
            cand.at[u],
            place(u, me),
            y_send.at[0, u],
            y_recv.at[0, u],
            device_id={"hist": partner},
            device_id_type=mesh_id,
        )
        copy.start()
        across[0, u] = copy
    loads[2].wait()
    spans = lax.broadcasted_iota(jnp.int32, (users, 128), 0)
    limits = jnp.zeros((users, 128), jnp.int32)
    for u in range(users):
        limits = jnp.where(spans == u, lengths[u], limits)
    lane = lax.broadcasted_iota(jnp.int32, (users, 128), 1)
    found = jnp.zeros((users, 128), jnp.int32)
    chosen = picks[...]
    for b in range(blocks):
        hit = jnp.max(jnp.where(chosen == me * blocks + b, 1.0, 0.0), axis=1, keepdims=True)
        found = jnp.where(jnp.logical_and(lane == b, hit > 0.0), 1, found)
    flags[...] = jnp.where((me * blocks + lane) * BLOCK < limits, found, 0)
    locals_[0].wait()
    for copy in weight_copies:
        copy.wait()
    key_weight, value_weight = all_proj[1], all_proj[2]
    shape = (blocks, BLOCK, embed)
    places = lax.broadcasted_iota(jnp.int32, shape, 0) * BLOCK + lax.broadcasted_iota(jnp.int32, shape, 1)
    places = places + me * own_rows
    for u in range(users):
        for k in range(line - 1):
            along[k, u].wait_recv()
            source = lax.rem(spot + line - (k + 1), line) * 2 + side
            copy = pltpu.make_async_remote_copy(
                place(u, source),
                place(u, source),
                y_send.at[k + 1, u],
                y_recv.at[k + 1, u],
                device_id={"hist": partner},
                device_id_type=mesh_id,
            )
            copy.start()
            across[k + 1, u] = copy
        fetches[u].wait()
        block_rows = rows_in[u].reshape(shape).astype(jnp.float32)
        alive = places < lengths[u]
        safe = jnp.where(alive, block_rows, block_rows[:, 0:1, :]).astype(jnp.bfloat16).reshape(own_rows, embed)
        kept = jnp.where(alive, block_rows, 0.0).astype(jnp.bfloat16).reshape(own_rows, embed)
        keys[u] = jnp.dot(safe, key_weight, preferred_element_type=jnp.float32).astype(jnp.bfloat16)
        values[u] = lax.dot_general(
            value_weight, kept, (((0,), (1,)), ((), ())), preferred_element_type=jnp.float32
        ).astype(jnp.bfloat16)
    for u in range(users):
        for k in range(line):
            across[k, u].wait_recv()
        locals_[1 + u].wait()
        query[u] = lax.dot_general(
            all_proj[0], all_cand[u], (((0,), (1,)), ((), ())), preferred_element_type=jnp.float32
        ).astype(jnp.bfloat16)
    for copy in list(along.values()) + list(across.values()):
        copy.wait_send()


def attend_kernel(
    own_cands,
    lengths,
    flags,
    base,
    query,
    keys,
    values,
    parts,
    stats,
    acc,
    shift,
    top,
    probs,
    slots,
    owners,
):
    users, embed, cands = query.shape
    head = embed // H
    tall = acc[0].shape[1]
    blocks = keys.shape[1] // BLOCK
    factor = math.log2(math.e) / math.sqrt(head)
    first = base[0]

    owners[0] = 0
    slots[0] = PAD
    slots[1] = PAD
    item = jnp.int32(1)
    begins, counts = [], []
    for u in range(users):
        last = jnp.int32(0)
        at = item * PAIR
        begins.append(item)
        for b in range(blocks):
            alive = flags[u, b]
            slots[at] = b
            at = at + alive
            last = jnp.where(alive > 0, b, last)
        for k in range(3 * PAIR):
            slots[at + k] = last + PAD
        for p in range(blocks // PAIR + 3):
            owners[item + p] = u
        counts.append(at - item * PAIR)
        item = (at + 1) // PAIR
    trips = (item - 1 + TRIP - 1) // TRIP

    def start_of(slot):
        block = jnp.where(slot >= PAD, slot - PAD, slot)
        return pl.multiple_of(block * BLOCK, BLOCK)

    column = lax.broadcasted_iota(jnp.int32, (1, embed), 1)
    mine = [jnp.where(column // head == h, 1.0, 0.0).astype(jnp.bfloat16) for h in range(H)]

    for u in range(users):
        sample = keys[u, pl.ds(start_of(slots[begins[u] * PAIR]), SAMPLE), :]
        guess = jnp.dot(
            jnp.concatenate([sample * mine[h] for h in range(H)], axis=0), query[u], preferred_element_type=jnp.float32
        )
        for h in range(H):
            most = jnp.max(guess[h * SAMPLE : (h + 1) * SAMPLE, :], axis=0, keepdims=True)
            shift[h][u] = most * factor
    for h in range(H):
        acc[h][...] = jnp.zeros(acc[h].shape, jnp.float32)
    for k in range(2):
        probs[2 + k][...] = jnp.zeros(probs[2 + k].shape, jnp.bfloat16)

    right = lax.broadcasted_iota(jnp.int32, (tall - head, BLOCK), 1)
    under = lax.broadcasted_iota(jnp.int32, (tall - head, BLOCK), 0)
    right = jnp.where(under == 0, right, jnp.iinfo(jnp.int32).max)

    def scores(i, h):
        user = owners[i]
        key = jnp.concatenate([keys[user, pl.ds(start_of(slots[i * PAIR + k]), BLOCK), :] for k in range(PAIR)], axis=0)
        got = jnp.dot(key * mine[h], query[user], preferred_element_type=jnp.float32)
        return got * factor - shift[h][user]

    def gain(i, h, prob):
        user = owners[i]
        pieces = []
        for k in range(PAIR):
            slot = slots[i * PAIR + k]
            start = start_of(slot)
            limit = jnp.where(slot >= PAD, 0, lengths[user] - (start + first * BLOCK))
            one = jnp.where(right < limit, 1.0, 0.0).astype(jnp.bfloat16)
            value = values[user, h * head : (h + 1) * head, pl.ds(start, BLOCK)]
            value = jnp.where(slot >= PAD, jnp.zeros_like(value), value)
            pieces.append(jnp.concatenate([value, one], axis=0))
        return jnp.dot(jnp.concatenate(pieces, axis=1), prob, preferred_element_type=jnp.float32)

    @pl.loop(0, trips)
    def _(step):
        begin = step * TRIP + 1
        for s in range(TRIP * H):
            late, head_late = begin + (s + 2 * H - LAG) // H - 2, (s + H - LAG) % H
            probs[s % 4][...] = jnp.exp2(scores(begin + s // H, s % H)).astype(jnp.bfloat16)
            acc[head_late][owners[late]] += gain(late, head_late, probs[(s - LAG) % 4][...])

    for k in range(LAG):
        h = H - LAG + k
        user = owners[trips * TRIP]
        acc[h][user] += gain(trips * TRIP, h, probs[(TRIP * H - LAG + k) % 4][...])

    wrong = jnp.zeros((1, cands), jnp.float32)
    for u in range(users):
        for h in range(H):
            amount = acc[h][u, head : head + 1, :]
            fine = jnp.logical_and(amount > SMALL, amount < LARGE)
            wrong = jnp.maximum(wrong, jnp.where(fine, 0.0, jnp.where(counts[u] > 0, 1.0, 0.0)))

    @pl.when(jnp.max(wrong) > 0.0)
    def _():
        for h in range(H):
            acc[h][...] = jnp.zeros(acc[h].shape, jnp.float32)
            top[h][...] = jnp.full(top[h].shape, LOW, jnp.float32)

        @pl.loop(1, item)
        def _(i):
            user = owners[i]
            for h in range(H):
                got = scores(i, h)
                before = top[h][user]
                peak = jnp.maximum(before, jnp.max(got, axis=0, keepdims=True))
                prob = jnp.exp2(got - peak).astype(jnp.bfloat16)
                acc[h][user] = acc[h][user] * jnp.exp2(before - peak) + gain(i, h, prob)
                top[h][user] = peak

        for h in range(H):
            shift[h][...] = shift[h][...] + top[h][...]

    means, logs = [], []
    for u in range(users):
        rows, row_logs = [], []
        for h in range(H):
            amount = acc[h][u, head : head + 1, :]
            some = jnp.logical_and(counts[u] > 0, amount > 0.0)
            safe = jnp.where(some, amount, 1.0)
            mean = jnp.where(some, acc[h][u, 0:head, :] * (1.0 / safe), 0.0)
            rows.append(mean.astype(jnp.bfloat16))
            row_logs.append(jnp.where(some, shift[h][u] + jnp.log2(safe), LOW))
        means.append(jnp.concatenate(rows, axis=0))
        logs.append(jnp.concatenate(row_logs, axis=0))
    pad = parts.shape[2] * LANES - users * own_cands
    for dest in range(2 * parts.shape[1]):
        at = slice(dest * own_cands, (dest + 1) * own_cands)
        for pieces, out in ((means, parts), (logs, stats)):
            row = [m[:, at] for m in pieces]
            if pad > 0:
                row.append(jnp.zeros((row[0].shape[0], pad), row[0].dtype))
            row = jnp.concatenate(row, axis=1)
            for c in range(parts.shape[2]):
                out[dest % 2, dest // 2, c] = row[:, c * LANES : (c + 1) * LANES]


def join(logs, means):
    heads, rows = logs[0].shape[0], means[0].shape[0] // logs[0].shape[0]
    highest = functools.reduce(jnp.maximum, logs)
    shares = [jnp.exp2(log - highest) for log in logs]
    total = functools.reduce(jnp.add, shares)
    shares = [share * (1.0 / total) for share in shares]
    pieces = []
    for h in range(heads):
        at = slice(h * rows, (h + 1) * rows)
        pieces.append(functools.reduce(jnp.add, [m[at, :] * w[h : h + 1, :] for m, w in zip(means, shares)]))
    return highest + jnp.log2(total), jnp.concatenate(pieces, axis=0)


def combine_kernel(
    n,
    parts,
    stats,
    out_weight,
    result,
    near,
    near_stats,
    mixed,
    mixed_stats,
    far,
    far_stats,
    y_send,
    y_recv,
    z_send,
    z_recv,
    zs_send,
    zs_recv,
):
    mesh_id = pl.DeviceIdType.MESH
    me = lax.axis_index("hist")
    line = n // 2
    side, spot = lax.rem(me, 2), me // 2
    partner = spot * 2 + (1 - side)
    chunks = parts.shape[2]
    target = [lax.rem(spot + k, line) for k in range(line)]
    barrier = pltpu.get_barrier_semaphore()
    for peer in [partner] + [target[k] * 2 + side for k in range(1, line)]:
        pl.semaphore_signal(barrier, inc=1, device_id={"hist": peer}, device_id_type=mesh_id)
    pl.semaphore_wait(barrier, line)
    order = sorted(range(1, line), key=lambda k: -min(k, line - k)) + [0]

    def across(src, dst, k):
        copy = pltpu.make_async_remote_copy(
            src, dst, y_send.at[k], y_recv.at[k], device_id={"hist": partner}, device_id_type=mesh_id
        )
        copy.start()
        return copy

    first = across(stats.at[1 - side], near_stats, line * chunks)
    crossing = {
        (k, c): across(parts.at[1 - side, target[k], c], near.at[target[k], c], k * chunks + c)
        for k in order
        for c in range(chunks)
    }
    first.wait_recv()
    along = {}
    own = []
    for k in order:
        for c in range(chunks):
            crossing[k, c].wait_recv()
            log, mean = join(
                [stats[side, target[k], c], near_stats[target[k], c]],
                [parts[side, target[k], c].astype(jnp.float32), near[target[k], c].astype(jnp.float32)],
            )
            if k == 0:
                own.append((log, mean))
                continue
            mixed_stats[k - 1, c] = log
            mixed[k - 1, c] = mean.astype(jnp.bfloat16)
            for src, dst, send, recv, kind in (
                (mixed_stats, far_stats, zs_send, zs_recv, 0),
                (mixed, far, z_send, z_recv, 1),
            ):
                copy = pltpu.make_async_remote_copy(
                    src.at[k - 1, c],
                    dst.at[k - 1, c],
                    send.at[k - 1, c],
                    recv.at[k - 1, c],
                    device_id={"hist": target[k] * 2 + side},
                    device_id_type=mesh_id,
                )
                copy.start()
                along[k, c, kind] = copy
    for c in range(chunks):
        logs, means = [own[c][0]], [own[c][1]]
        for k in order[:-1]:
            along[k, c, 0].wait_recv()
            along[k, c, 1].wait_recv()
            logs.append(far_stats[k - 1, c])
            means.append(far[k - 1, c].astype(jnp.float32))
        _, attended = join(logs, means)
        result[c * LANES : (c + 1) * LANES, :] = lax.dot_general(
            attended.astype(jnp.bfloat16),
            out_weight[3],
            (((0,), (0,)), ((), ())),
            preferred_element_type=jnp.float32,
        ).astype(jnp.bfloat16)
    for copy in [first] + list(crossing.values()) + list(along.values()):
        copy.wait_send()


def body(candidates, history, projections, lengths, selected):
    n = lax.axis_size("hist")
    ranks = lax.axis_size("dp")
    candidates, history, projections, lengths, selected = (
        pltpu.with_memory_space_constraint(x, pltpu.HBM) for x in (candidates, history, projections, lengths, selected)
    )
    users, own_cands, embed = candidates.shape
    cands = n * own_cands
    line = n // 2
    own_rows = history.shape[1]
    blocks = own_rows // BLOCK
    first = (lax.axis_index("hist") * blocks).astype(jnp.int32)
    base = first.reshape(1)
    weights, query, keys, values, flags = pl.pallas_call(
        functools.partial(gather_kernel, n, ranks),
        out_shape=[
            pltpu.VMEM((projections.shape[0], ranks * projections.shape[1], embed), jnp.bfloat16),
            pltpu.VMEM((users, embed, cands), jnp.bfloat16),
            pltpu.VMEM((users, own_rows, embed), jnp.bfloat16),
            pltpu.VMEM((users, embed, own_rows), jnp.bfloat16),
            jax.ShapeDtypeStruct((users, 128), jnp.int32),
        ],
        in_specs=[pl.BlockSpec(memory_space=pltpu.SMEM)] + [pl.BlockSpec(memory_space=pltpu.HBM)] * 4,
        out_specs=[pl.BlockSpec(memory_space=pltpu.VMEM)] * 5,
        scratch_shapes=[
            pltpu.VMEM(candidates.shape, jnp.bfloat16),
            pltpu.VMEM(projections.shape, jnp.bfloat16),
            pltpu.VMEM(selected.shape, jnp.int32),
            pltpu.VMEM((users, cands, embed), jnp.bfloat16),
            pltpu.VMEM((users, own_rows, embed), jnp.bfloat16),
            pltpu.SemaphoreType.DMA((users + 1,)),
            pltpu.SemaphoreType.DMA((3,)),
            pltpu.SemaphoreType.DMA((users,)),
            pltpu.SemaphoreType.DMA((line - 1, users)),
            pltpu.SemaphoreType.DMA((line - 1, users)),
            pltpu.SemaphoreType.DMA((line, users)),
            pltpu.SemaphoreType.DMA((line, users)),
            pltpu.SemaphoreType.DMA((ranks - 1,)),
            pltpu.SemaphoreType.DMA((ranks - 1,)),
        ],
        compiler_params=pltpu.CompilerParams(collective_id=1, has_side_effects=True, vmem_limit_bytes=ROOM),
        name="gather",
    )(lengths, candidates, projections, history, selected)
    chunks = -(-users * own_cands // LANES)
    wide = chunks * LANES
    parts, stats = pl.pallas_call(
        functools.partial(attend_kernel, own_cands),
        in_specs=[pl.BlockSpec(memory_space=pltpu.SMEM)] * 3 + [pl.BlockSpec(memory_space=pltpu.VMEM)] * 3,
        out_specs=[pl.BlockSpec(memory_space=pltpu.VMEM)] * 2,
        scratch_shapes=[
            [pltpu.VMEM((users, embed // H + 16, cands), jnp.float32)] * H,
            [pltpu.VMEM((users, 1, cands), jnp.float32)] * H,
            [pltpu.VMEM((users, 1, cands), jnp.float32)] * H,
            [pltpu.VMEM((PAIR * BLOCK, cands), jnp.bfloat16)] * 4,
            pltpu.SMEM(((users * blocks) + users * PAIR + 8 * PAIR,), jnp.int32),
            pltpu.SMEM((users * (blocks // PAIR + 1) + 8,), jnp.int32),
        ],
        out_shape=[
            pltpu.VMEM((2, line, chunks, embed, LANES), jnp.bfloat16),
            pltpu.VMEM((2, line, chunks, H, LANES), jnp.float32),
        ],
        compiler_params=pltpu.CompilerParams(vmem_limit_bytes=ROOM),
        name="attend",
    )(lengths, flags, base, query, keys, values)
    result = pl.pallas_call(
        functools.partial(combine_kernel, n),
        out_shape=jax.ShapeDtypeStruct((wide, embed), jnp.bfloat16),
        in_specs=[pl.BlockSpec(memory_space=pltpu.VMEM)] * 3,
        out_specs=pl.BlockSpec(memory_space=pltpu.VMEM),
        scratch_shapes=[
            pltpu.VMEM((line, chunks, embed, LANES), jnp.bfloat16),
            pltpu.VMEM((line, chunks, H, LANES), jnp.float32),
            pltpu.VMEM((line - 1, chunks, embed, LANES), jnp.bfloat16),
            pltpu.VMEM((line - 1, chunks, H, LANES), jnp.float32),
            pltpu.VMEM((line - 1, chunks, embed, LANES), jnp.bfloat16),
            pltpu.VMEM((line - 1, chunks, H, LANES), jnp.float32),
        ]
        + [pltpu.SemaphoreType.DMA((line * chunks + 1,))] * 2
        + [pltpu.SemaphoreType.DMA((line - 1, chunks))] * 4,
        compiler_params=pltpu.CompilerParams(collective_id=0, has_side_effects=True, vmem_limit_bytes=ROOM),
        name="combine",
    )(parts, stats, weights)
    return result[: users * own_cands].reshape(users, own_cands, embed)


def solution(mesh):
    placed = (
        P("dp", "hist", None),
        P("dp", "hist", None),
        P(None, "dp", None),
        P("dp"),
        P("dp", None),
    )
    return jax.shard_map(
        body, mesh=mesh, in_specs=placed, out_specs=P("dp", "hist", None), check_vma=False
    )
```
